32 devices in a mesh: batch: 16 (over z, y, core), rep: 2 (over x).
Axes of the slice: x: 2, y: 2, z: 4, core: 2. Of those that a mesh axis runs over, the one named last changes fastest.
Arguments:
- queries: bfloat16 [2048, 512], P('batch', 'rep'), may hold values from -8 to 8
- passages: bfloat16 [2048, 512], P('batch', 'rep'), may hold values from -8 to 8
- positives: int32 [2048], replicated, may hold values from 0 to 2047, each once
Outputs:
- grad_queries: float32 [2048, 512], P('batch', 'rep')
- grad_passages: float32 [2048, 512], P('batch', 'rep')
The draws below stay inside these ranges and needn't reach their ends.
Inputs may be any that keep to these rules, and one draw needn't show every extreme that they name: `positives`: each passage is the positive of exactly one query.
All inputs are finite; a program needn't handle non-finite values.
Results may differ from the reference program's by a relative error of at most 0.0013.
Values may be sent and summed in bfloat16 or wider, within the bound.
A program may use at most 128 MiB of HBM per device.

```python
import math
import jax
import jax.numpy as jnp
from jax import lax

D = 512
TOTAL = 2048


def embedding_draw(key, member):
    member_key = jax.random.fold_in(key, member + 11)
    scale_key, entry_key = jax.random.split(member_key, 2)
    row_scale = jnp.exp(jax.random.uniform(scale_key, (TOTAL, 1), jnp.float32, math.log(0.3), math.log(3.0)))
    entries = jax.random.normal(entry_key, (TOTAL, D), jnp.float32)
    values = jnp.clip(row_scale * entries, -8.0, 8.0)
    return values.astype(jnp.bfloat16)


def draw_queries(key, part):
    return embedding_draw(key, 0)


def draw_passages(key, part):
    return embedding_draw(key, 1)


def setup_inputs(seed: int = 0) -> dict:
    key_list = jax.random.split(jax.random.key(seed), 4)
    return {
        "queries": draw_queries(jax.random.fold_in(key_list[3], 71), 0),
        "passages": draw_passages(jax.random.fold_in(key_list[3], 71), 0),
        "positives": jax.random.permutation(key_list[2], TOTAL).astype(jnp.int32),
    }


def block_scores(query_block, passages, logit_scale):
    return jnp.dot(query_block, passages.T, preferred_element_type=jnp.float32) * logit_scale

def reference(queries, passages, positives):
    logit_scale = 1.0 / math.sqrt(D)
    block_rows = math.gcd(TOTAL, 512)
    block_count = TOTAL // block_rows
    query_blocks = queries.reshape(block_count, block_rows, D)
    positive_blocks = positives.reshape(block_count, block_rows)

    def first_sweep(running, query_block):
        column_high, column_total = running
        scores = block_scores(query_block, passages, logit_scale)
        row_high = lax.optimization_barrier(jnp.max(scores, axis=1))
        row_norm = row_high + jnp.log(lax.optimization_barrier(jnp.sum(jnp.exp(scores - row_high[:, None]), axis=1)))
        new_high = jnp.maximum(column_high, lax.optimization_barrier(jnp.max(scores, axis=0)))
        column_total = column_total * jnp.exp(column_high - new_high) + lax.optimization_barrier(jnp.sum(jnp.exp(scores - new_high[None, :]), axis=0))
        return ((new_high, column_total), row_norm)
    starting = (jnp.full((TOTAL,), -1e+30, jnp.float32), jnp.zeros((TOTAL,), jnp.float32))
    (column_high, column_total), row_norms = lax.scan(first_sweep, starting, query_blocks)
    column_norms = column_high + jnp.log(column_total)
    passage_ids = jnp.arange(TOTAL, dtype=jnp.int32)

    def second_sweep(grad_passages, inputs):
        query_block, row_block, positive_block = inputs
        scores = block_scores(query_block, passages, logit_scale)
        matches = (positive_block[:, None] == passage_ids[None, :]).astype(jnp.float32)
        weights = jnp.exp(scores - row_block[:, None]) + jnp.exp(scores - column_norms[None, :]) - 2.0 * matches
        weights = weights.astype(jnp.bfloat16)
        grad_block = jnp.dot(weights, passages, preferred_element_type=jnp.float32) * logit_scale
        grad_passages = grad_passages + jnp.dot(weights.T, query_block, preferred_element_type=jnp.float32) * logit_scale
        return (grad_passages, grad_block)
    grad_passages, grad_blocks = lax.scan(second_sweep, jnp.zeros((TOTAL, D), jnp.float32), (query_blocks, row_norms, positive_blocks))
    return (grad_blocks.reshape(TOTAL, D), grad_passages)
```

```python
import functools
import math

import jax
import jax.numpy as jnp
from jax import lax
from jax.experimental import pallas as pl
from jax.experimental.pallas import tpu as pltpu
from jax.sharding import PartitionSpec as P

MESH = pl.DeviceIdType.MESH
F32 = jnp.float32
BF16 = jnp.bfloat16
I16 = jnp.int16


def dot(a, b, da, db):
    return lax.dot_general(a, b, (((da,), (db,)), ((), ())), preferred_element_type=F32)


def as_column(row, lanes):
    return jnp.broadcast_to(row, (lanes, row.shape[1])).T


def kernel(
    Z,
    scale,
    q_ref,
    p_ref,
    pos_hbm,
    gq_ref,
    gp_ref,
    Q,
    Qs,
    PB,
    S,
    W,
    Ws,
    rst,
    rrc,
    cst,
    crc,
    PM,
    pos_ref,
    gqp,
    gqt,
    gqr,
    gqk,
    gqkr,
    gpt,
    gpr,
    gpk,
    gpkr,
    near,
    line,
    rest,
    in_s,
    q_s,
    q_r,
    p_s,
    p_r,
    f_s,
    f_r,
    h_s,
    h_r,
    r_s,
    r_r,
    c_s,
    c_r,
    w_s,
    w_r,
    gq_s,
    gq_r,
    gp_s,
    gp_r,
    gqk_s,
    gqk_r,
    gpk_s,
    gpk_r,
):
    n, w = q_ref.shape
    b = lax.axis_index("batch")
    x = lax.axis_index("rep")
    z, y, c = b // 4, (b // 2) % 2, b % 2
    rows, cols = 2 * n, Z * n
    blocks = min(Z, 4)
    wide = blocks * n
    chunks = Z // blocks

    def dev(zz, yy, cc, xx):
        return (zz * 4 + yy * 2 + cc, xx)

    def plane(j):
        xx = 1 - x if j & 1 else x
        yy = 1 - y if j & 2 else y
        return xx, yy

    def remote(src, dst, s, r, device):
        return pltpu.make_async_remote_copy(
            src_ref=src, dst_ref=dst, send_sem=s, recv_sem=r, device_id=device, device_id_type=MESH
        )

    def span(k, size):
        return pl.ds(k * size if isinstance(k, int) else pl.multiple_of(k * size, size), size)

    def up(dz):
        return (z + dz) % Z

    own = c == x
    crossed = jnp.logical_not(own)
    sibling = dev(z, y, 1 - c, x)

    def target(zz):
        return dev(zz, y, x, c)

    barrier = pltpu.get_barrier_semaphore()

    q_own = Q.at[x, span(y, n)]
    p_in = pltpu.make_async_copy(p_ref, PM, in_s.at[0])
    q_in = pltpu.make_async_copy(q_ref, q_own, in_s.at[1])
    pos_in = pltpu.make_async_copy(pos_hbm, pos_ref, in_s.at[2])
    q_in.start()
    p_in.start()
    pos_in.start()

    def greet(sem, device):
        pl.semaphore_signal(sem, inc=1, device_id=device, device_id_type=MESH)

    place = 2 * y + x
    pairs = []
    for j in (1, 2, 3):
        xx, yy = plane(j)
        pairs.append((2 * yy + xx < place, dev(z, yy, c, xx), near.at[j - 1]))
    pairs.append((c == 0, sibling, rest))
    for dz in range(1, Z):
        zz = up(dz)
        pairs.append((zz < z, target(zz), line.at[z]))
        for cc in (0, 1):
            pairs.append((zz < z, dev(zz, y, cc, x), rest))
    first = jnp.logical_and(crossed, c < x)
    last = jnp.logical_and(crossed, c > x)
    for earlier, device, _ in pairs:

        @pl.when(jnp.logical_not(earlier))
        def _():
            greet(barrier, device)

    @pl.when(last)
    def _():
        greet(barrier, target(z))

    greetings = place + 3 * z + (1 - c) + first.astype(jnp.int32)

    @pl.when(greetings > 0)
    def _():
        pl.semaphore_wait(barrier, greetings)

    for earlier, device, sem in pairs:

        @pl.when(earlier)
        def _():
            greet(sem, device)

    @pl.when(first)
    def _():
        greet(line.at[z], target(z))

    p_in.wait()
    p_block = PB.at[x, span(z, n)]

    def p_copy(zz):
        return remote(PM, p_block, p_s, p_r.at[z], target(zz))

    for k in range(Z - 1):

        @pl.when(k < z)
        def _():
            p_copy(k).start()

    q_in.wait()
    pos_in.wait()

    @pl.when(own)
    def _():
        PB[c, span(z, n), :] = PM[...]

    q_copies = []
    for j in (1, 3, 2):
        xx, yy = plane(j)
        q_copies.append(remote(q_own, q_own, q_s, q_r, dev(z, yy, c, xx)))

        @pl.when(2 * yy + xx > place)
        def _():
            pl.semaphore_wait(near.at[j - 1], 1)

        q_copies[-1].start()

    @pl.when(last)
    def _():
        pl.semaphore_wait(line.at[z], 1)

    @pl.when(crossed)
    def _():
        p_copy(z).start()

    for k in range(1, Z):

        @pl.when(k > z)
        def _():
            pl.semaphore_wait(line.at[k], 1)
            p_copy(k).start()

    answers = 2 * (Z - 1 - z) + c

    @pl.when(answers > 0)
    def _():
        pl.semaphore_wait(rest, answers)

    def part(zz):
        return PB.at[c, span(zz, n)]

    def forward(zz):
        return remote(part(zz), part(zz), f_s, f_r.at[zz], sibling)

    def nth(k):
        return lax.select(k < z, z - 1 - k, jnp.int32(k))

    def score(k):
        zz = nth(k)
        forward(zz).wait_recv()
        at = span(zz, n)
        s = (dot(Q[0], PB[0, at, :], 1, 1) + dot(Q[1], PB[1, at, :], 1, 1)) * scale
        S[:, at] = s
        top = jnp.max(s, axis=0, keepdims=True)
        cst[:, at] = top
        cst[:, span(zz + Z, n)] = jnp.sum(jnp.exp(s - top), axis=0, keepdims=True)

    half = remote(Q.at[1 - c], Qs, h_s, h_r, sibling)

    @pl.when(own)
    def _():
        forward(z).start()

    def arrive(k):
        zz = nth(k)

        @pl.when(jnp.logical_or(zz != z, crossed))
        def _():
            pltpu.make_async_copy(PM, part(zz), p_r.at[zz]).wait()
            forward(zz).start()

    arrive(0)
    arrive(1)
    pltpu.make_async_copy(gqr, gqr, q_r).wait()
    half.start()
    for k in range(2, Z):
        if k < Z - 1:
            score(k - 2)
        arrive(k)
    for k in range(Z - 3, Z):
        score(k)

    col_copies = []
    for dz in range(Z):
        for dc in (0, 1):
            if dz or dc:
                k = dz * 2 + dc
                col_copies.append(
                    remote(cst, crc.at[k - 1], c_s, c_r, dev(up(dz), y, 1 - c if dc else c, x))
                )
                col_copies[-1].start()

    def row_high(k, high):
        return jnp.maximum(high, jnp.max(S[:, span(k, wide)], axis=1, keepdims=True))

    def row_total(k, total):
        s = S[:, span(k, wide)]
        return total + jnp.sum(jnp.exp(s - highest), axis=1, keepdims=True)

    low, zero = jnp.full((rows, 1), -1e30, F32), jnp.zeros((rows, 1), F32)
    if chunks == 1:
        highest = row_high(0, low)
        running = (highest, row_total(0, zero))
    else:
        highest = lax.fori_loop(0, chunks, row_high, low)
        running = (highest, lax.fori_loop(0, chunks, row_total, zero))

    def as_row(column):
        return jnp.broadcast_to(column, (rows, 128)).T[0:1, :]

    rst[:, 0:rows] = as_row(running[0])
    rst[:, rows : 2 * rows] = as_row(running[1])
    row_copies = []
    for j in (1, 2, 3):
        xx, yy = plane(j)
        row_copies.append(remote(rst, rrc.at[j - 1], r_s, r_r, dev(z, yy, c, xx)))
        row_copies[-1].start()

    places = jnp.concatenate(
        [
            as_column(pos_ref[pl.ds(z * 4 + yy * 2 + c, 1), :].astype(F32), 128)
            for yy in (0, 1)
        ],
        axis=0,
    )

    pltpu.make_async_copy(rrc, rrc, r_r).wait()
    high = rst[:, 0:rows]
    for j in range(3):
        high = jnp.maximum(high, rrc[j, :, 0:rows])
    total = rst[:, rows : 2 * rows] * jnp.exp(rst[:, 0:rows] - high)
    for j in range(3):
        total += rrc[j, :, rows : 2 * rows] * jnp.exp(rrc[j, :, 0:rows] - high)
    row_norm = as_column(high + jnp.log(total), 128)

    pltpu.make_async_copy(crc, crc, c_r).wait()
    high = cst[:, 0:cols]
    for k in range(2 * Z - 1):
        high = jnp.maximum(high, crc[k, :, 0:cols])
    total = cst[:, cols : 2 * cols] * jnp.exp(cst[:, 0:cols] - high)
    for k in range(2 * Z - 1):
        total += crc[k, :, cols : 2 * cols] * jnp.exp(crc[k, :, 0:cols] - high)
    col_norms = high + jnp.log(total)

    lane = lax.broadcasted_iota(jnp.int32, (rows, n), 1).astype(F32)

    shares = []
    for k in range(Z):
        at = span(k, n)
        s = S[:, at]
        col_norm = col_norms[:, k * n : (k + 1) * n]
        base = lax.convert_element_type((k * 4 + y * 2 + x) * n, F32)
        hit = jnp.where(places - lane == base, 2.0, 0.0)
        W[k] = (jnp.exp(s - row_norm) + jnp.exp(s - col_norm) - hit).astype(BF16)
        shares.append(remote(W.at[k], Ws.at[k], w_s, w_r.at[k], sibling))
        shares[-1].start()

    def pack(value):
        top = jnp.maximum(jnp.max(jnp.abs(value), axis=0, keepdims=True), 1e-30)
        return jnp.round(value * (32766.0 / top)).astype(jnp.int32).astype(I16), top * (1.0 / 32766.0)

    def unpack(at, step, k):
        return at[k].astype(jnp.int32).astype(F32) * step[k]

    def query_terms(h):
        def term(k):
            return dot(W[k], PB[h, span(k, n), :], 1, 0)

        if Z <= 4:
            return sum(term(k) for k in range(1, Z)) + term(0)
        return lax.fori_loop(0, Z, lambda k, t: t + term(k), jnp.zeros((rows, w), F32))

    for h in (0, 1):
        gqp[h] = query_terms(h)

    for yy, xx in ((0, 0), (0, 1), (1, 0), (1, 1)):

        @pl.when(jnp.logical_or(yy != y, xx != x))
        def _():
            j = (x + xx) % 2 + 2 * ((y + yy) % 2) - 1
            gqt[j], gqk[j] = pack(gqp[xx, yy * n : (yy + 1) * n, :])
            device = dev(z, yy, c, xx)
            remote(gqt.at[j], gqr.at[j], gq_s, gq_r, device).start()
            remote(gqk.at[j], gqkr.at[j], gqk_s, gqk_r, device).start()

    half.wait_recv()
    for k in range(Z):
        shares[k].wait_recv()
        packed, step = pack(dot(W[k], Q[c], 0, 0) + dot(Ws[k], Qs[...], 0, 0))
        away = jnp.logical_or(z != k, crossed)

        @pl.when(away)
        def _():
            gpt[k], gpk[k] = packed, step
            remote(gpt.at[k], gpr.at[z], gp_s, gp_r, target(k)).start()
            remote(gpk.at[k], gpkr.at[z], gpk_s, gpk_r, target(k)).start()

        @pl.when(jnp.logical_not(away))
        def _():
            gpr[k], gpkr[k] = packed, step

    pltpu.make_async_copy(gqr, gqr, gq_r).wait()
    pltpu.make_async_copy(gqkr, gqkr, gqk_r).wait()
    total = gqp[x, span(y, n), :]
    for j in range(3):
        total += unpack(gqr, gqkr, j)
    gq_ref[...] = total

    def gp_wait(count, data, step):
        pltpu.make_async_copy(gpr.at[pl.ds(0, count)], gpr.at[pl.ds(0, count)], data).wait()
        pltpu.make_async_copy(gpkr.at[pl.ds(0, count)], gpkr.at[pl.ds(0, count)], step).wait()

    def per_count(body):
        @pl.when(own)
        def _():
            body(Z - 1)

        @pl.when(crossed)
        def _():
            body(Z)

    per_count(lambda count: gp_wait(count, gp_r, gpk_r))
    gp_ref[...] = sum(unpack(gpr, gpkr, k) for k in range(Z))

    def p_wait(count):
        pltpu.make_async_copy(PB.at[0, pl.ds(0, count * n)], PB.at[0, pl.ds(0, count * n)], p_s).wait()
        gp_wait(count, gp_s, gpk_s)

    per_count(p_wait)
    for ref, sem in (
        (gqr, q_s),
        (PB.at[0], f_s),
        (W, w_s),
        (crc, c_s),
        (rrc, r_s),
        (gqt, gq_s),
        (gqk, gqk_s),
        (Qs, h_s),
    ):
        pltpu.make_async_copy(ref, ref, sem).wait()


def local(queries, passages, positives):
    n, w = queries.shape
    batch_count = lax.axis_size("batch")
    Z = batch_count // 4
    scale = 1.0 / math.sqrt(w * lax.axis_size("rep"))
    rows, cols = 2 * n, Z * n
    vmem = pl.BlockSpec(memory_space=pltpu.VMEM)
    dma = pltpu.SemaphoreType.DMA
    regular = pltpu.SemaphoreType.REGULAR
    hbm = pl.BlockSpec(memory_space=pltpu.HBM)
    operands = (queries, passages, positives.reshape(batch_count, n))
    grad_queries, grad_passages = pl.pallas_call(
        functools.partial(kernel, Z, scale),
        out_shape=(
            jax.ShapeDtypeStruct((n, w), F32),
            jax.ShapeDtypeStruct((n, w), F32),
        ),
        in_specs=[hbm] * 3,
        out_specs=(vmem, vmem),
        scratch_shapes=[
            pltpu.VMEM((2, rows, w), BF16),
            pltpu.VMEM((rows, w), BF16),
            pltpu.VMEM((2, cols, w), BF16),
            pltpu.VMEM((rows, cols), F32),
            pltpu.VMEM((Z, rows, n), BF16),
            pltpu.VMEM((Z, rows, n), BF16),
            pltpu.VMEM((1, 2 * rows), F32),
            pltpu.VMEM((3, 1, 2 * rows), F32),
            pltpu.VMEM((1, 2 * cols), F32),
            pltpu.VMEM((2 * Z - 1, 1, 2 * cols), F32),
            pltpu.VMEM((n, w), BF16),
            pltpu.VMEM((batch_count, n), jnp.int32),
            pltpu.VMEM((2, rows, w), F32),
            pltpu.VMEM((3, n, w), I16),
            pltpu.VMEM((3, n, w), I16),
            pltpu.VMEM((3, 1, w), F32),
            pltpu.VMEM((3, 1, w), F32),
            pltpu.VMEM((Z, n, w), I16),
            pltpu.VMEM((Z, n, w), I16),
            pltpu.VMEM((Z, 1, w), F32),
            pltpu.VMEM((Z, 1, w), F32),
            regular((3,)),
            regular((Z,)),
            regular,
            dma((3,)),
            dma,
            dma,
            dma,
            dma((Z,)),
            dma,
            dma((Z,)),
            dma,
            dma,
            dma,
            dma,
            dma,
            dma,
            dma,
            dma((Z,)),
            dma,
            dma,
            dma,
            dma,
            dma,
            dma,
            dma,
            dma,
        ],
        compiler_params=pltpu.CompilerParams(collective_id=0, has_side_effects=True, vmem_limit_bytes=6 * 2**20 + 40 * rows * cols),
    )(*(pltpu.with_memory_space_constraint(a, pltpu.HBM) for a in operands))
    return grad_queries * scale, grad_passages * scale


def solution(mesh):
    in_specs = (P("batch", "rep"), P("batch", "rep"), P())
    out_specs = (P("batch", "rep"), P("batch", "rep"))
    return jax.shard_map(local, mesh=mesh, in_specs=in_specs, out_specs=out_specs, check_vma=False)
```

```python
import functools
import math

import jax
import jax.numpy as jnp
from jax import lax
from jax.experimental import pallas as pl
from jax.experimental.pallas import tpu as pltpu
from jax.sharding import PartitionSpec as P

MESH = pl.DeviceIdType.MESH
F32 = jnp.float32
BF16 = jnp.bfloat16
I16 = jnp.int16


def dot(a, b, da, db):
    return lax.dot_general(a, b, (((da,), (db,)), ((), ())), preferred_element_type=F32)


def as_column(row, lanes):
    return jnp.broadcast_to(row, (lanes, row.shape[1])).T


def kernel(
    Z,
    scale,
    q_ref,
    p_ref,
    pos_hbm,
    gq_ref,
    gp_ref,
    Q,
    Qs,
    PB,
    S,
    W,
    Ws,
    rst,
    rrc,
    cst,
    crc,
    PM,
    pos_ref,
    gqp,
    gqt,
    gqr,
    gqk,
    gqkr,
    gpt,
    gpr,
    gpk,
    gpkr,
    near,
    line,
    rest,
    in_s,
    q_s,
    q_r,
    p_s,
    p_r,
    f_s,
    f_r,
    h_s,
    h_r,
    r_s,
    r_r,
    c_s,
    c_r,
    w_s,
    w_r,
    gq_s,
    gq_r,
    gp_s,
    gp_r,
    gqk_s,
    gqk_r,
    gpk_s,
    gpk_r,
):
    n, w = q_ref.shape
    b = lax.axis_index("batch")
    x = lax.axis_index("rep")
    z, y, c = b // 4, (b // 2) % 2, b % 2
    rows, cols = 2 * n, Z * n
    blocks = min(Z, 4)
    wide = blocks * n
    chunks = Z // blocks

    def dev(zz, yy, cc, xx):
        return (zz * 4 + yy * 2 + cc, xx)

    def plane(j):
        xx = 1 - x if j & 1 else x
        yy = 1 - y if j & 2 else y
        return xx, yy

    def remote(src, dst, s, r, device):
        return pltpu.make_async_remote_copy(
            src_ref=src, dst_ref=dst, send_sem=s, recv_sem=r, device_id=device, device_id_type=MESH
        )

    def span(k, size):
        return pl.ds(k * size if isinstance(k, int) else pl.multiple_of(k * size, size), size)

    def up(dz):
        return (z + dz) % Z

    own = c == x
    crossed = jnp.logical_not(own)
    sibling = dev(z, y, 1 - c, x)

    def target(zz):
        return dev(zz, y, x, c)

    barrier = pltpu.get_barrier_semaphore()

    q_own = Q.at[x, span(y, n)]
    p_in = pltpu.make_async_copy(p_ref, PM, in_s.at[0])
    q_in = pltpu.make_async_copy(q_ref, q_own, in_s.at[1])
    pos_in = pltpu.make_async_copy(pos_hbm, pos_ref, in_s.at[2])
    q_in.start()
    p_in.start()
    pos_in.start()

    def greet(sem, device):
        pl.semaphore_signal(sem, inc=1, device_id=device, device_id_type=MESH)

    place = 2 * y + x
    pairs = []
    for j in (1, 2, 3):
        xx, yy = plane(j)
        pairs.append((2 * yy + xx < place, dev(z, yy, c, xx), near.at[j - 1]))
    pairs.append((c == 0, sibling, rest))
    for dz in range(1, Z):
        zz = up(dz)
        pairs.append((zz < z, target(zz), line.at[z]))
        for cc in (0, 1):
            pairs.append((zz < z, dev(zz, y, cc, x), rest))
    first = jnp.logical_and(crossed, c < x)
    last = jnp.logical_and(crossed, c > x)
    for earlier, device, _ in pairs:

        @pl.when(jnp.logical_not(earlier))
        def _():
            greet(barrier, device)

    @pl.when(last)
    def _():
        greet(barrier, target(z))

    greetings = place + 3 * z + (1 - c) + first.astype(jnp.int32)

    @pl.when(greetings > 0)
    def _():
        pl.semaphore_wait(barrier, greetings)

    for earlier, device, sem in pairs:

        @pl.when(earlier)
        def _():
            greet(sem, device)

    @pl.when(first)
    def _():
        greet(line.at[z], target(z))

    p_in.wait()
    p_block = PB.at[x, span(z, n)]

    def p_copy(zz):
        return remote(PM, p_block, p_s, p_r.at[z], target(zz))

    for k in range(Z - 1):

        @pl.when(k < z)
        def _():
            p_copy(k).start()

    q_in.wait()
    pos_in.wait()

    @pl.when(own)
    def _():
        PB[c, span(z, n), :] = PM[...]

    q_copies = []
    for j in (1, 3, 2):
        xx, yy = plane(j)
        q_copies.append(remote(q_own, q_own, q_s, q_r, dev(z, yy, c, xx)))

        @pl.when(2 * yy + xx > place)
        def _():
            pl.semaphore_wait(near.at[j - 1], 1)

        q_copies[-1].start()

    @pl.when(last)
    def _():
        pl.semaphore_wait(line.at[z], 1)

    @pl.when(crossed)
    def _():
        p_copy(z).start()

    def send_later(zz):
        pl.semaphore_wait(line.at[zz], 1)
        p_copy(zz).start()

    for k in range(2, Z):

        @pl.when(k > z + 1)
        def _():
            send_later(k)

    @pl.when(z < Z - 1)
    def _():
        send_later(z + 1)

    answers = 2 * (Z - 1 - z) + c

    @pl.when(answers > 0)
    def _():
        pl.semaphore_wait(rest, answers)

    def part(zz):
        return PB.at[c, span(zz, n)]

    def forward(zz):
        return remote(part(zz), part(zz), f_s, f_r.at[zz], sibling)

    def nth(k):
        return lax.select(k < Z - z, z + k, jnp.int32(Z - 1 - k))

    def scores(*ks):
        for k in ks:
            forward(nth(k)).wait_recv()
        for k in ks:
            zz = nth(k)
            at = span(zz, n)
            s = (dot(Q[0], PB[0, at, :], 1, 1) + dot(Q[1], PB[1, at, :], 1, 1)) * scale
            S[:, at] = s
            top = jnp.max(s, axis=0, keepdims=True)
            cst[:, at] = top
            cst[:, span(zz + Z, n)] = jnp.sum(jnp.exp(s - top), axis=0, keepdims=True)

    half = remote(Q.at[1 - c], Qs, h_s, h_r, sibling)

    @pl.when(own)
    def _():
        forward(z).start()

    def arrive(k):
        zz = nth(k)

        @pl.when(jnp.logical_or(zz != z, crossed))
        def _():
            pltpu.make_async_copy(PM, part(zz), p_r.at[zz]).wait()
            forward(zz).start()

    arrive(0)
    arrive(1)
    pltpu.make_async_copy(gqr, gqr, q_r).wait()
    half.start()
    scores(0, 1)
    for k in range(2, Z):
        arrive(k)
    for k in range(2, Z, 2):
        scores(k, k + 1)

    col_copies = []
    for dz in range(Z):
        for dc in (0, 1):
            if dz or dc:
                k = dz * 2 + dc
                col_copies.append(
                    remote(cst, crc.at[k - 1], c_s, c_r, dev(up(dz), y, 1 - c if dc else c, x))
                )
                col_copies[-1].start()

    def row_high(k, high):
        return jnp.maximum(high, jnp.max(S[:, span(k, wide)], axis=1, keepdims=True))

    def row_total(k, total):
        s = S[:, span(k, wide)]
        return total + jnp.sum(jnp.exp(s - highest), axis=1, keepdims=True)

    low, zero = jnp.full((rows, 1), -1e30, F32), jnp.zeros((rows, 1), F32)
    if chunks == 1:
        highest = row_high(0, low)
        running = (highest, row_total(0, zero))
    else:
        highest = lax.fori_loop(0, chunks, row_high, low)
        running = (highest, lax.fori_loop(0, chunks, row_total, zero))

    def as_row(column):
        return jnp.broadcast_to(column, (rows, 128)).T[0:1, :]

    rst[:, 0:rows] = as_row(running[0])
    rst[:, rows : 2 * rows] = as_row(running[1])
    row_copies = []
    for j in (1, 2, 3):
        xx, yy = plane(j)
        row_copies.append(remote(rst, rrc.at[j - 1], r_s, r_r, dev(z, yy, c, xx)))
        row_copies[-1].start()

    places = jnp.concatenate(
        [
            as_column(pos_ref[pl.ds(z * 4 + yy * 2 + c, 1), :].astype(F32), 128)
            for yy in (0, 1)
        ],
        axis=0,
    )

    pltpu.make_async_copy(rrc, rrc, r_r).wait()
    high = rst[:, 0:rows]
    for j in range(3):
        high = jnp.maximum(high, rrc[j, :, 0:rows])
    total = rst[:, rows : 2 * rows] * jnp.exp(rst[:, 0:rows] - high)
    for j in range(3):
        total += rrc[j, :, rows : 2 * rows] * jnp.exp(rrc[j, :, 0:rows] - high)
    row_norm = as_column(high + jnp.log(total), 128)

    pltpu.make_async_copy(crc, crc, c_r).wait()
    high = cst[:, 0:cols]
    for k in range(2 * Z - 1):
        high = jnp.maximum(high, crc[k, :, 0:cols])
    total = cst[:, cols : 2 * cols] * jnp.exp(cst[:, 0:cols] - high)
    for k in range(2 * Z - 1):
        total += crc[k, :, cols : 2 * cols] * jnp.exp(crc[k, :, 0:cols] - high)
    col_norms = high + jnp.log(total)

    lane = lax.broadcasted_iota(jnp.int32, (rows, n), 1).astype(F32)

    shares = []
    for k in range(Z):
        at = span(k, n)
        s = S[:, at]
        col_norm = col_norms[:, k * n : (k + 1) * n]
        base = lax.convert_element_type((k * 4 + y * 2 + x) * n, F32)
        hit = jnp.where(places - lane == base, 2.0, 0.0)
        W[k] = (jnp.exp(s - row_norm) + jnp.exp(s - col_norm) - hit).astype(BF16)
        shares.append(remote(W.at[k], Ws.at[k], w_s, w_r.at[k], sibling))
        shares[-1].start()

    def pack(value):
        top = jnp.maximum(jnp.max(jnp.abs(value), axis=0, keepdims=True), 1e-30)
        return jnp.round(value * (32766.0 / top)).astype(jnp.int32).astype(I16), top * (1.0 / 32766.0)

    def unpack(at, step, k):
        return at[k].astype(jnp.int32).astype(F32) * step[k]

    def query_terms(h):
        def term(k):
            return dot(W[k], PB[h, span(k, n), :], 1, 0)

        if Z <= 4:
            return sum(term(k) for k in range(1, Z)) + term(0)
        return lax.fori_loop(0, Z, lambda k, t: t + term(k), jnp.zeros((rows, w), F32))

    for h in (0, 1):
        gqp[h] = query_terms(h)

    def gq_send(yy, xx):
        j = (x + xx) % 2 + 2 * ((y + yy) % 2) - 1
        gqt[j], gqk[j] = pack(gqp[xx, yy * n : (yy + 1) * n, :])
        device = dev(z, yy, c, xx)
        remote(gqt.at[j], gqr.at[j], gq_s, gq_r, device).start()
        remote(gqk.at[j], gqkr.at[j], gqk_s, gqk_r, device).start()

    quarters = ((0, 0), (0, 1), (1, 0), (1, 1))
    for yy, xx in quarters:

        @pl.when(jnp.logical_and(yy != y, xx == x))
        def _():
            gq_send(yy, xx)

    half.wait_recv()

    def gp_send(k):
        shares[k].wait_recv()
        packed, step = pack(dot(W[k], Q[c], 0, 0) + dot(Ws[k], Qs[...], 0, 0))
        away = jnp.logical_or(z != k, crossed)

        @pl.when(away)
        def _():
            gpt[k], gpk[k] = packed, step
            remote(gpt.at[k], gpr.at[z], gp_s, gp_r, target(k)).start()
            remote(gpk.at[k], gpkr.at[z], gpk_s, gpk_r, target(k)).start()

        @pl.when(jnp.logical_not(away))
        def _():
            gpr[k], gpkr[k] = packed, step

    gp_send(0)
    for yy, xx in quarters:

        @pl.when(xx != x)
        def _():
            gq_send(yy, xx)

    for k in range(1, Z):
        gp_send(k)

    pltpu.make_async_copy(gqr, gqr, gq_r).wait()
    pltpu.make_async_copy(gqkr, gqkr, gqk_r).wait()
    total = gqp[x, span(y, n), :]
    for j in range(3):
        total += unpack(gqr, gqkr, j)
    gq_ref[...] = total

    def gp_wait(count, data, step):
        pltpu.make_async_copy(gpr.at[pl.ds(0, count)], gpr.at[pl.ds(0, count)], data).wait()
        pltpu.make_async_copy(gpkr.at[pl.ds(0, count)], gpkr.at[pl.ds(0, count)], step).wait()

    def per_count(body):
        @pl.when(own)
        def _():
            body(Z - 1)

        @pl.when(crossed)
        def _():
            body(Z)

    per_count(lambda count: gp_wait(count, gp_r, gpk_r))
    gp_ref[...] = sum(unpack(gpr, gpkr, k) for k in range(Z))

    def p_wait(count):
        pltpu.make_async_copy(PB.at[0, pl.ds(0, count * n)], PB.at[0, pl.ds(0, count * n)], p_s).wait()
        gp_wait(count, gp_s, gpk_s)

    per_count(p_wait)
    for ref, sem in (
        (gqr, q_s),
        (PB.at[0], f_s),
        (W, w_s),
        (crc, c_s),
        (rrc, r_s),
        (gqt, gq_s),
        (gqk, gqk_s),
        (Qs, h_s),
    ):
        pltpu.make_async_copy(ref, ref, sem).wait()


def local(queries, passages, positives):
    n, w = queries.shape
    batch_count = lax.axis_size("batch")
    Z = batch_count // 4
    scale = 1.0 / math.sqrt(w * lax.axis_size("rep"))
    rows, cols = 2 * n, Z * n
    vmem = pl.BlockSpec(memory_space=pltpu.VMEM)
    dma = pltpu.SemaphoreType.DMA
    regular = pltpu.SemaphoreType.REGULAR
    hbm = pl.BlockSpec(memory_space=pltpu.HBM)
    operands = (queries, passages, positives.reshape(batch_count, n))
    grad_queries, grad_passages = pl.pallas_call(
        functools.partial(kernel, Z, scale),
        out_shape=(
            jax.ShapeDtypeStruct((n, w), F32),
            jax.ShapeDtypeStruct((n, w), F32),
        ),
        in_specs=[hbm] * 3,
        out_specs=(vmem, vmem),
        scratch_shapes=[
            pltpu.VMEM((2, rows, w), BF16),
            pltpu.VMEM((rows, w), BF16),
            pltpu.VMEM((2, cols, w), BF16),
            pltpu.VMEM((rows, cols), F32),
            pltpu.VMEM((Z, rows, n), BF16),
            pltpu.VMEM((Z, rows, n), BF16),
            pltpu.VMEM((1, 2 * rows), F32),
            pltpu.VMEM((3, 1, 2 * rows), F32),
            pltpu.VMEM((1, 2 * cols), F32),
            pltpu.VMEM((2 * Z - 1, 1, 2 * cols), F32),
            pltpu.VMEM((n, w), BF16),
            pltpu.VMEM((batch_count, n), jnp.int32),
            pltpu.VMEM((2, rows, w), F32),
            pltpu.VMEM((3, n, w), I16),
            pltpu.VMEM((3, n, w), I16),
            pltpu.VMEM((3, 1, w), F32),
            pltpu.VMEM((3, 1, w), F32),
            pltpu.VMEM((Z, n, w), I16),
            pltpu.VMEM((Z, n, w), I16),
            pltpu.VMEM((Z, 1, w), F32),
            pltpu.VMEM((Z, 1, w), F32),
            regular((3,)),
            regular((Z,)),
            regular,
            dma((3,)),
            dma,
            dma,
            dma,
            dma((Z,)),
            dma,
            dma((Z,)),
            dma,
            dma,
            dma,
            dma,
            dma,
            dma,
            dma,
            dma((Z,)),
            dma,
            dma,
            dma,
            dma,
            dma,
            dma,
            dma,
            dma,
        ],
        compiler_params=pltpu.CompilerParams(collective_id=0, has_side_effects=True, vmem_limit_bytes=6 * 2**20 + 40 * rows * cols),
    )(*(pltpu.with_memory_space_constraint(a, pltpu.HBM) for a in operands))
    return grad_queries * scale, grad_passages * scale


def solution(mesh):
    in_specs = (P("batch", "rep"), P("batch", "rep"), P())
    out_specs = (P("batch", "rep"), P("batch", "rep"))
    return jax.shard_map(local, mesh=mesh, in_specs=in_specs, out_specs=out_specs, check_vma=False)
```

```python
import functools
import math

import jax
import jax.numpy as jnp
from jax import lax
from jax.experimental import pallas as pl
from jax.experimental.pallas import tpu as pltpu
from jax.sharding import PartitionSpec as P

MESH = pl.DeviceIdType.MESH
F32 = jnp.float32
BF16 = jnp.bfloat16
I16 = jnp.int16
TURNS = ((0, 1, 3, 2), (0, 3, 2, 1), (0, 3, 1, 2), (0, 2, 1, 3))


def dot(a, b, da, db):
    return lax.dot_general(a, b, (((da,), (db,)), ((), ())), preferred_element_type=F32)


def as_column(row, lanes):
    return jnp.broadcast_to(row, (lanes, row.shape[1])).T


def kernel(
    Z,
    scale,
    q_ref,
    p_ref,
    pos_hbm,
    gq_ref,
    gp_ref,
    Q,
    Qs,
    PB,
    S,
    A,
    W,
    Ws,
    rst,
    rrc,
    cst,
    crc,
    PM,
    pos_ref,
    gqp,
    gqt,
    gqr,
    gqk,
    gqkr,
    gpt,
    gpr,
    gpk,
    gpkr,
    near,
    line,
    rest,
    in_s,
    q_s,
    q_r,
    p_s,
    p_r,
    f_s,
    f_r,
    h_s,
    h_r,
    r_s,
    r_r,
    c_s,
    c_r,
    w_s,
    w_r,
    gq_s,
    gq_r,
    gp_s,
    gp_r,
    gqk_s,
    gqk_r,
    gpk_s,
    gpk_r,
):
    n, w = q_ref.shape
    b = lax.axis_index("batch")
    x = lax.axis_index("rep")
    z, y, c = b // 4, (b // 2) % 2, b % 2
    rows, cols = 2 * n, Z * n

    def dev(zz, yy, cc, xx):
        return (zz * 4 + yy * 2 + cc, xx)

    def plane(j):
        xx = 1 - x if j & 1 else x
        yy = 1 - y if j & 2 else y
        return xx, yy

    def remote(src, dst, s, r, device):
        return pltpu.make_async_remote_copy(
            src_ref=src, dst_ref=dst, send_sem=s, recv_sem=r, device_id=device, device_id_type=MESH
        )

    def span(k, size):
        return pl.ds(k * size if isinstance(k, int) else pl.multiple_of(k * size, size), size)

    def up(dz):
        return (z + dz) % Z

    own = c == 1 - x
    crossed = jnp.logical_not(own)
    sibling = dev(z, y, 1 - c, x)

    def target(zz):
        return dev(zz, y, 1 - x, 1 - c)

    barrier = pltpu.get_barrier_semaphore()

    q_own = Q.at[x, span(y, n)]
    p_in = pltpu.make_async_copy(p_ref, PM, in_s.at[0])
    q_in = pltpu.make_async_copy(q_ref, q_own, in_s.at[1])
    pos_in = pltpu.make_async_copy(pos_hbm, pos_ref, in_s.at[2])
    q_in.start()
    p_in.start()
    pos_in.start()

    def greet(sem, device):
        pl.semaphore_signal(sem, inc=1, device_id=device, device_id_type=MESH)

    place = 2 * y + x
    pairs = []
    for j in (1, 2, 3):
        xx, yy = plane(j)
        pairs.append((2 * yy + xx < place, dev(z, yy, c, xx), near.at[j - 1]))
    pairs.append((c == 0, sibling, rest))
    for dz in range(1, Z):
        zz = up(dz)
        pairs.append((zz < z, target(zz), line.at[z]))
        for cc in (0, 1):
            pairs.append((zz < z, dev(zz, y, cc, x), rest))
    first = jnp.logical_and(crossed, x == 1)
    last = jnp.logical_and(crossed, x == 0)
    for earlier, device, _ in pairs:

        @pl.when(jnp.logical_not(earlier))
        def _():
            greet(barrier, device)

    @pl.when(last)
    def _():
        greet(barrier, target(z))

    greetings = place + 3 * z + (1 - c) + first.astype(jnp.int32)

    @pl.when(greetings > 0)
    def _():
        pl.semaphore_wait(barrier, greetings)

    for earlier, device, sem in pairs:

        @pl.when(earlier)
        def _():
            greet(sem, device)

    @pl.when(first)
    def _():
        greet(line.at[z], target(z))

    p_in.wait()
    p_block = PB.at[x, span(z, n)]

    def p_copy(zz):
        return remote(PM, p_block, p_s, p_r.at[z], target(zz))

    @pl.when(first)
    def _():
        p_copy(z).start()

    for k in range(Z - 1):

        @pl.when(k < z)
        def _():
            p_copy(k).start()

    q_in.wait()
    pos_in.wait()

    @pl.when(own)
    def _():
        PB[x, span(z, n), :] = PM[...]

    @pl.when(last)
    def _():
        pl.semaphore_wait(line.at[z], 1)
        p_copy(z).start()

    q_copies = []
    for j in (1, 3, 2):
        xx, yy = plane(j)
        q_copies.append(remote(q_own, q_own, q_s, q_r, dev(z, yy, c, xx)))

        @pl.when(2 * yy + xx > place)
        def _():
            pl.semaphore_wait(near.at[j - 1], 1)

        q_copies[-1].start()

    def send_later(zz):
        pl.semaphore_wait(line.at[zz], 1)
        p_copy(zz).start()

    @pl.when(jnp.logical_and(z > 0, z < Z - 1))
    def _():
        send_later(z + 1)

    for k in range(2, Z):

        @pl.when(k > z + 1)
        def _():
            send_later(k)

    @pl.when(z == 0)
    def _():
        send_later(1)

    answers = 2 * (Z - 1 - z) + c

    @pl.when(answers > 0)
    def _():
        pl.semaphore_wait(rest, answers)

    def part(zz):
        return PB.at[1 - c, span(zz, n)]

    def forward(zz):
        return remote(part(zz), part(zz), f_s, f_r.at[zz], sibling)

    def nth(k):
        return lax.select(k < Z - z, z + k, jnp.int32(Z - 1 - k))

    def scores(*ks):
        for k in ks:
            forward(nth(k)).wait_recv()
        parts = []
        for k in ks:
            zz = nth(k)
            at = span(zz, n)
            s = (dot(Q[0], PB[0, at, :], 1, 1) + dot(Q[1], PB[1, at, :], 1, 1)) * scale
            S[:, at] = s
            top = jnp.max(s, axis=0, keepdims=True)
            cst[:, at] = top
            cst[:, span(zz + Z, n)] = jnp.sum(jnp.exp(s - top), axis=0, keepdims=True)
            parts.append(s)
        return parts

    def row_part(parts, running):
        high = jnp.max(functools.reduce(jnp.maximum, parts), axis=1, keepdims=True)
        if running is not None:
            high = jnp.maximum(high, running[0])
        total = jnp.sum(sum(jnp.exp(s - high) for s in parts), axis=1, keepdims=True)
        if running is not None:
            total += running[1] * jnp.exp(running[0] - high)
        return high, total

    half = remote(Q.at[c], Qs, h_s, h_r, sibling)

    @pl.when(own)
    def _():
        forward(z).start()

    def arrive(k):
        zz = nth(k)

        @pl.when(jnp.logical_or(zz != z, crossed))
        def _():
            pltpu.make_async_copy(PM, part(zz), p_r.at[zz]).wait()
            forward(zz).start()

    for k in range(Z):
        arrive(k)
    pltpu.make_async_copy(gqr, gqr, q_r).wait()
    half.start()
    running = None
    for k in range(0, Z - 2, 2):
        running = row_part(scores(k, k + 1), running)
    parts = scores(Z - 2, Z - 1)

    col_copies = []
    for dz in range(Z):
        for dc in (0, 1):
            if dz or dc:
                k = dz * 2 + dc
                col_copies.append(
                    remote(cst, crc.at[k - 1], c_s, c_r, dev(up(dz), y, 1 - c if dc else c, x))
                )
                col_copies[-1].start()

    running = row_part(parts, running)

    def as_row(column):
        return jnp.broadcast_to(column, (rows, 128)).T[0:1, :]

    rst[:, 0:rows] = as_row(running[0])
    rst[:, rows : 2 * rows] = as_row(running[1])
    row_copies = []
    for j in (1, 2, 3):
        xx, yy = plane(j)
        row_copies.append(remote(rst, rrc.at[j - 1], r_s, r_r, dev(z, yy, c, xx)))
        row_copies[-1].start()

    places = jnp.concatenate(
        [
            as_column(pos_ref[pl.ds(z * 4 + yy * 2 + c, 1), :].astype(F32), 128)
            for yy in (0, 1)
        ],
        axis=0,
    )

    pltpu.make_async_copy(rrc, rrc, r_r).wait()
    high = rst[:, 0:rows]
    for j in range(3):
        high = jnp.maximum(high, rrc[j, :, 0:rows])
    total = rst[:, rows : 2 * rows] * jnp.exp(rst[:, 0:rows] - high)
    for j in range(3):
        total += rrc[j, :, rows : 2 * rows] * jnp.exp(rrc[j, :, 0:rows] - high)
    row_norm = as_column(high + jnp.log(total), 128)

    lane = lax.broadcasted_iota(jnp.int32, (rows, n), 1).astype(F32)
    for k in range(Z):
        base = lax.convert_element_type((k * 4 + y * 2 + 1 - x) * n, F32)
        hit = jnp.where(places - lane == base, 2.0, 0.0)
        A[k] = jnp.exp(S[:, span(k, n)] - row_norm) - hit

    pltpu.make_async_copy(crc, crc, c_r).wait()
    high = cst[:, 0:cols]
    for k in range(2 * Z - 1):
        high = jnp.maximum(high, crc[k, :, 0:cols])
    total = cst[:, cols : 2 * cols] * jnp.exp(cst[:, 0:cols] - high)
    for k in range(2 * Z - 1):
        total += crc[k, :, cols : 2 * cols] * jnp.exp(crc[k, :, 0:cols] - high)
    crc[0, :, 0:cols] = high + jnp.log(total)

    def turn(i):
        if Z != 4:
            return jnp.int32(i)
        first_z, second_z, third_z, fourth_z = (row[i] for row in TURNS)
        low = lax.select(z == 0, jnp.int32(first_z), jnp.int32(second_z))
        high = lax.select(z == 2, jnp.int32(third_z), jnp.int32(fourth_z))
        return lax.select(z < 2, low, high)

    def share(k):
        return remote(W.at[k], Ws.at[k], w_s, w_r.at[k], sibling)

    for i in range(Z):
        k = turn(i)
        W[k] = (A[k] + jnp.exp(S[:, span(k, n)] - crc[0, :, span(k, n)])).astype(BF16)
        share(k).start()

    def pack(value):
        top = jnp.maximum(jnp.max(jnp.abs(value), axis=0, keepdims=True), 1e-30)
        return jnp.round(value * (32766.0 / top)).astype(jnp.int32).astype(I16), top * (1.0 / 32766.0)

    def unpack(at, step, k):
        return at[k].astype(jnp.int32).astype(F32) * step[k]

    def query_terms(h):
        def term(k):
            return dot(W[k], PB[h, span(k, n), :], 1, 0)

        if Z <= 4:
            return dot(jnp.concatenate([W[k] for k in range(Z)], axis=1), PB[h], 1, 0)
        return lax.fori_loop(0, Z, lambda k, t: t + term(k), jnp.zeros((rows, w), F32))

    def gq_send(yy, xx):
        j = (x + xx) % 2 + 2 * ((y + yy) % 2) - 1
        gqt[j], gqk[j] = pack(gqp[xx, yy * n : (yy + 1) * n, :])
        device = dev(z, yy, c, xx)
        remote(gqt.at[j], gqr.at[j], gq_s, gq_r, device).start()
        remote(gqk.at[j], gqkr.at[j], gqk_s, gqk_r, device).start()

    for h in (0, 1):
        gqp[h] = query_terms(h)
    for yy, xx in ((0, 0), (0, 1), (1, 0), (1, 1)):

        @pl.when(jnp.logical_or(yy != y, xx != x))
        def _():
            gq_send(yy, xx)

    half.wait_recv()

    for i in range(Z):
        k = turn(i)
        mine = dot(W[k], Q[1 - c], 0, 0)
        share(k).wait_recv()
        packed, step = pack(mine + dot(Ws[k], Qs[...], 0, 0))
        away = jnp.logical_or(z != k, crossed)

        @pl.when(away)
        def _():
            gpt[k], gpk[k] = packed, step
            remote(gpt.at[k], gpr.at[z], gp_s, gp_r, target(k)).start()
            remote(gpk.at[k], gpkr.at[z], gpk_s, gpk_r, target(k)).start()

        @pl.when(jnp.logical_not(away))
        def _():
            gpr[k], gpkr[k] = packed, step

    pltpu.make_async_copy(gqr, gqr, gq_r).wait()
    pltpu.make_async_copy(gqkr, gqkr, gqk_r).wait()
    total = gqp[x, span(y, n), :]
    for j in range(3):
        total += unpack(gqr, gqkr, j)
    gq_ref[...] = total

    def gp_wait(count, data, step):
        pltpu.make_async_copy(gpr.at[pl.ds(0, count)], gpr.at[pl.ds(0, count)], data).wait()
        pltpu.make_async_copy(gpkr.at[pl.ds(0, count)], gpkr.at[pl.ds(0, count)], step).wait()

    def per_count(body):
        @pl.when(own)
        def _():
            body(Z - 1)

        @pl.when(crossed)
        def _():
            body(Z)

    per_count(lambda count: gp_wait(count, gp_r, gpk_r))
    gp_ref[...] = sum(unpack(gpr, gpkr, k) for k in range(Z))

    def p_wait(count):
        pltpu.make_async_copy(PB.at[0, pl.ds(0, count * n)], PB.at[0, pl.ds(0, count * n)], p_s).wait()
        gp_wait(count, gp_s, gpk_s)

    per_count(p_wait)
    for ref, sem in (
        (gqr, q_s),
        (PB.at[0], f_s),
        (W, w_s),
        (crc, c_s),
        (rrc, r_s),
        (gqt, gq_s),
        (gqk, gqk_s),
        (Qs, h_s),
    ):
        pltpu.make_async_copy(ref, ref, sem).wait()


def local(queries, passages, positives):
    n, w = queries.shape
    batch_count = lax.axis_size("batch")
    Z = batch_count // 4
    scale = 1.0 / math.sqrt(w * lax.axis_size("rep"))
    rows, cols = 2 * n, Z * n
    vmem = pl.BlockSpec(memory_space=pltpu.VMEM)
    dma = pltpu.SemaphoreType.DMA
    regular = pltpu.SemaphoreType.REGULAR
    hbm = pl.BlockSpec(memory_space=pltpu.HBM)
    operands = (queries, passages, positives.reshape(batch_count, n))
    grad_queries, grad_passages = pl.pallas_call(
        functools.partial(kernel, Z, scale),
        out_shape=(
            jax.ShapeDtypeStruct((n, w), F32),
            jax.ShapeDtypeStruct((n, w), F32),
        ),
        in_specs=[hbm] * 3,
        out_specs=(vmem, vmem),
        scratch_shapes=[
            pltpu.VMEM((2, rows, w), BF16),
            pltpu.VMEM((rows, w), BF16),
            pltpu.VMEM((2, cols, w), BF16),
            pltpu.VMEM((rows, cols), F32),
            pltpu.VMEM((Z, rows, n), F32),
            pltpu.VMEM((Z, rows, n), BF16),
            pltpu.VMEM((Z, rows, n), BF16),
            pltpu.VMEM((1, 2 * rows), F32),
            pltpu.VMEM((3, 1, 2 * rows), F32),
            pltpu.VMEM((1, 2 * cols), F32),
            pltpu.VMEM((2 * Z - 1, 1, 2 * cols), F32),
            pltpu.VMEM((n, w), BF16),
            pltpu.VMEM((batch_count, n), jnp.int32),
            pltpu.VMEM((2, rows, w), F32),
            pltpu.VMEM((3, n, w), I16),
            pltpu.VMEM((3, n, w), I16),
            pltpu.VMEM((3, 1, w), F32),
            pltpu.VMEM((3, 1, w), F32),
            pltpu.VMEM((Z, n, w), I16),
            pltpu.VMEM((Z, n, w), I16),
            pltpu.VMEM((Z, 1, w), F32),
            pltpu.VMEM((Z, 1, w), F32),
            regular((3,)),
            regular((Z,)),
            regular,
            dma((3,)),
            dma,
            dma,
            dma,
            dma((Z,)),
            dma,
            dma((Z,)),
            dma,
            dma,
            dma,
            dma,
            dma,
            dma,
            dma,
            dma((Z,)),
            dma,
            dma,
            dma,
            dma,
            dma,
            dma,
            dma,
            dma,
        ],
        compiler_params=pltpu.CompilerParams(collective_id=0, has_side_effects=True, vmem_limit_bytes=6 * 2**20 + 40 * rows * cols),
    )(*(pltpu.with_memory_space_constraint(a, pltpu.HBM) for a in operands))
    return grad_queries * scale, grad_passages * scale


def solution(mesh):
    in_specs = (P("batch", "rep"), P("batch", "rep"), P())
    out_specs = (P("batch", "rep"), P("batch", "rep"))
    return jax.shard_map(local, mesh=mesh, in_specs=in_specs, out_specs=out_specs, check_vma=False)
```

```python
import functools
import math

import jax
import jax.numpy as jnp
from jax import lax
from jax.experimental import pallas as pl
from jax.experimental.pallas import tpu as pltpu
from jax.sharding import PartitionSpec as P

MESH = pl.DeviceIdType.MESH
F32 = jnp.float32
BF16 = jnp.bfloat16
I16 = jnp.int16
TURNS = ((0, 1, 3, 2), (0, 3, 2, 1), (0, 3, 1, 2), (0, 2, 1, 3))


def dot(a, b, da, db):
    return lax.dot_general(a, b, (((da,), (db,)), ((), ())), preferred_element_type=F32)


def as_column(row, lanes):
    return jnp.broadcast_to(row, (lanes, row.shape[1])).T


def kernel(
    Z,
    scale,
    q_ref,
    p_ref,
    pos_hbm,
    gq_ref,
    gp_ref,
    Q,
    Qs,
    PB,
    S,
    A,
    W,
    Ws,
    rst,
    rrc,
    cst,
    crc,
    PM,
    pos_ref,
    gqp,
    gqt,
    gqr,
    gqk,
    gqkr,
    gpt,
    gpr,
    gpk,
    gpkr,
    near,
    line,
    rest,
    in_s,
    q_s,
    q_r,
    p_s,
    p_r,
    f_s,
    f_r,
    h_s,
    h_r,
    r_s,
    r_r,
    c_s,
    c_r,
    w_s,
    w_r,
    gq_s,
    gq_r,
    gp_s,
    gp_r,
    gqk_s,
    gqk_r,
    gpk_s,
    gpk_r,
    d_r,
    dk_r,
):
    n, w = q_ref.shape
    b = lax.axis_index("batch")
    x = lax.axis_index("rep")
    z, y, c = b // 4, (b // 2) % 2, b % 2
    rows, cols = 2 * n, Z * n

    def dev(zz, yy, cc, xx):
        return (zz * 4 + yy * 2 + cc, xx)

    def plane(j):
        xx = 1 - x if j & 1 else x
        yy = 1 - y if j & 2 else y
        return xx, yy

    def remote(src, dst, s, r, device):
        return pltpu.make_async_remote_copy(
            src_ref=src, dst_ref=dst, send_sem=s, recv_sem=r, device_id=device, device_id_type=MESH
        )

    def span(k, size):
        return pl.ds(k * size if isinstance(k, int) else pl.multiple_of(k * size, size), size)

    def up(dz):
        return (z + dz) % Z

    own = c == 1 - x
    crossed = jnp.logical_not(own)
    sibling = dev(z, y, 1 - c, x)

    def target(zz):
        return dev(zz, y, 1 - x, 1 - c)

    barrier = pltpu.get_barrier_semaphore()

    q_own = Q.at[x, span(y, n)]
    p_in = pltpu.make_async_copy(p_ref, PM, in_s.at[0])
    q_in = pltpu.make_async_copy(q_ref, q_own, in_s.at[1])
    pos_in = pltpu.make_async_copy(pos_hbm, pos_ref, in_s.at[2])
    q_in.start()
    p_in.start()
    pos_in.start()

    def greet(sem, device):
        pl.semaphore_signal(sem, inc=1, device_id=device, device_id_type=MESH)

    place = 2 * y + x
    pairs = []
    for j in (1, 2):
        xx, yy = plane(j)
        pairs.append((2 * yy + xx < place, dev(z, yy, c, xx), near.at[j - 1]))
    pairs.append((c == 0, sibling, rest))
    for dz in range(1, Z):
        zz = up(dz)
        pairs.append((zz < z, target(zz), line.at[z]))
        for cc in (0, 1):
            pairs.append((zz < z, dev(zz, y, cc, x), rest))
    first = jnp.logical_and(crossed, x == 1)
    last = jnp.logical_and(crossed, x == 0)
    for earlier, device, _ in pairs:

        @pl.when(jnp.logical_not(earlier))
        def _():
            greet(barrier, device)

    @pl.when(last)
    def _():
        greet(barrier, target(z))

    greetings = x + y + 3 * z + (1 - c) + first.astype(jnp.int32)

    @pl.when(greetings > 0)
    def _():
        pl.semaphore_wait(barrier, greetings)

    for earlier, device, sem in pairs:

        @pl.when(earlier)
        def _():
            greet(sem, device)

    @pl.when(first)
    def _():
        greet(line.at[z], target(z))

    p_in.wait()
    p_block = PB.at[x, span(z, n)]

    def p_copy(zz):
        return remote(PM, p_block, p_s, p_r.at[z], target(zz))

    @pl.when(first)
    def _():
        p_copy(z).start()

    for k in range(Z - 1):

        @pl.when(k < z)
        def _():
            p_copy(k).start()

    q_in.wait()
    pos_in.wait()

    @pl.when(own)
    def _():
        PB[x, span(z, n), :] = PM[...]

    @pl.when(last)
    def _():
        pl.semaphore_wait(line.at[z], 1)
        p_copy(z).start()

    q_copies = []
    for j in (1, 2):
        xx, yy = plane(j)
        q_copies.append(remote(q_own, q_own, q_s, q_r.at[j - 1], dev(z, yy, c, xx)))

        @pl.when(2 * yy + xx > place)
        def _():
            pl.semaphore_wait(near.at[j - 1], 1)

        q_copies[-1].start()

    def send_later(zz):
        pl.semaphore_wait(line.at[zz], 1)
        p_copy(zz).start()

    @pl.when(jnp.logical_and(z > 0, z < Z - 1))
    def _():
        send_later(z + 1)

    for k in range(2, Z):

        @pl.when(k > z + 1)
        def _():
            send_later(k)

    @pl.when(z == 0)
    def _():
        send_later(1)

    answers = 2 * (Z - 1 - z) + c

    @pl.when(answers > 0)
    def _():
        pl.semaphore_wait(rest, answers)

    q_copies[0].wait_recv()
    q_far = Q.at[1 - x, span(y, n)]
    remote(q_far, q_far, q_s, q_r.at[1], dev(z, 1 - y, c, x)).start()

    def part(zz):
        return PB.at[1 - c, span(zz, n)]

    def forward(zz):
        return remote(part(zz), part(zz), f_s, f_r.at[zz], sibling)

    def nth(k):
        return lax.select(k < Z - z, z + k, jnp.int32(Z - 1 - k))

    def scores(*ks):
        for k in ks:
            forward(nth(k)).wait_recv()
        parts = []
        for k in ks:
            zz = nth(k)
            at = span(zz, n)
            s = (dot(Q[0], PB[0, at, :], 1, 1) + dot(Q[1], PB[1, at, :], 1, 1)) * scale
            S[:, at] = s
            top = jnp.max(s, axis=0, keepdims=True)
            cst[:, at] = top
            cst[:, span(zz + Z, n)] = jnp.sum(jnp.exp(s - top), axis=0, keepdims=True)
            parts.append(s)
        return parts

    def row_part(parts, running):
        high = jnp.max(functools.reduce(jnp.maximum, parts), axis=1, keepdims=True)
        if running is not None:
            high = jnp.maximum(high, running[0])
        total = jnp.sum(sum(jnp.exp(s - high) for s in parts), axis=1, keepdims=True)
        if running is not None:
            total += running[1] * jnp.exp(running[0] - high)
        return high, total

    half = remote(Q.at[c], Qs, h_s, h_r, sibling)

    @pl.when(own)
    def _():
        forward(z).start()

    def arrive(k):
        zz = nth(k)

        @pl.when(jnp.logical_or(zz != z, crossed))
        def _():
            pltpu.make_async_copy(PM, part(zz), p_r.at[zz]).wait()
            forward(zz).start()

    for k in range(Z):
        arrive(k)
    pltpu.make_async_copy(Q.at[0], Q.at[0], q_r.at[1]).wait()
    half.start()
    running = None
    for k in range(0, Z - 2, 2):
        running = row_part(scores(k, k + 1), running)
    parts = scores(Z - 2, Z - 1)

    col_copies = []
    for dz in range(Z):
        for dc in (0, 1):
            if dz or dc:
                k = dz * 2 + dc
                col_copies.append(
                    remote(cst, crc.at[k - 1], c_s, c_r, dev(up(dz), y, 1 - c if dc else c, x))
                )
                col_copies[-1].start()

    running = row_part(parts, running)

    def as_row(column):
        return jnp.broadcast_to(column, (rows, 128)).T[0:1, :]

    rst[:, 0:rows] = as_row(running[0])
    rst[:, rows : 2 * rows] = as_row(running[1])
    row_copies = []
    for j in (1, 2, 3):
        xx, yy = plane(j)
        row_copies.append(remote(rst, rrc.at[j - 1], r_s, r_r, dev(z, yy, c, xx)))
        row_copies[-1].start()

    places = jnp.concatenate(
        [
            as_column(pos_ref[pl.ds(z * 4 + yy * 2 + c, 1), :].astype(F32), 128)
            for yy in (0, 1)
        ],
        axis=0,
    )

    pltpu.make_async_copy(rrc, rrc, r_r).wait()
    high = rst[:, 0:rows]
    for j in range(3):
        high = jnp.maximum(high, rrc[j, :, 0:rows])
    total = rst[:, rows : 2 * rows] * jnp.exp(rst[:, 0:rows] - high)
    for j in range(3):
        total += rrc[j, :, rows : 2 * rows] * jnp.exp(rrc[j, :, 0:rows] - high)
    row_norm = as_column(high + jnp.log(total), 128)

    lane = lax.broadcasted_iota(jnp.int32, (rows, n), 1).astype(F32)
    for k in range(Z):
        base = lax.convert_element_type((k * 4 + y * 2 + 1 - x) * n, F32)
        hit = jnp.where(places - lane == base, 2.0, 0.0)
        A[k] = jnp.exp(S[:, span(k, n)] - row_norm) - hit

    pltpu.make_async_copy(crc, crc, c_r).wait()
    high = cst[:, 0:cols]
    for k in range(2 * Z - 1):
        high = jnp.maximum(high, crc[k, :, 0:cols])
    total = cst[:, cols : 2 * cols] * jnp.exp(cst[:, 0:cols] - high)
    for k in range(2 * Z - 1):
        total += crc[k, :, cols : 2 * cols] * jnp.exp(crc[k, :, 0:cols] - high)
    crc[0, :, 0:cols] = high + jnp.log(total)

    def turn(i):
        if Z != 4:
            return jnp.int32(i)
        first_z, second_z, third_z, fourth_z = (row[i] for row in TURNS)
        low = lax.select(z == 0, jnp.int32(first_z), jnp.int32(second_z))
        high = lax.select(z == 2, jnp.int32(third_z), jnp.int32(fourth_z))
        return lax.select(z < 2, low, high)

    def share(k):
        return remote(W.at[k], Ws.at[k], w_s, w_r.at[k], sibling)

    for i in range(Z):
        k = turn(i)
        W[k] = (A[k] + jnp.exp(S[:, span(k, n)] - crc[0, :, span(k, n)])).astype(BF16)
        share(k).start()

    def pack(value):
        top = jnp.maximum(jnp.max(jnp.abs(value), axis=0, keepdims=True), 1e-30)
        return jnp.round(value * (32766.0 / top)).astype(jnp.int32).astype(I16), top * (1.0 / 32766.0)

    def unpack(at, step, k):
        return at[k].astype(jnp.int32).astype(F32) * step[k]

    def query_terms(h):
        def term(k):
            return dot(W[k], PB[h, span(k, n), :], 1, 0)

        if Z <= 4:
            return dot(jnp.concatenate([W[k] for k in range(Z)], axis=1), PB[h], 1, 0)
        return lax.fori_loop(0, Z, lambda k, t: t + term(k), jnp.zeros((rows, w), F32))

    def gq_send(j, value, slot, data, step, device):
        gqt[j], gqk[j] = pack(value)
        remote(gqt.at[j], gqr.at[slot], gq_s, data, device).start()
        remote(gqk.at[j], gqkr.at[slot], gqk_s, step, device).start()

    for h in (0, 1):
        gqp[h] = query_terms(h)
    beside, across = dev(z, 1 - y, c, x), dev(z, y, c, 1 - x)
    corner = dev(z, 1 - y, c, lax.select(c == 1, x, 1 - x))

    def gq_across(more):
        gq_send(2, gqp[1 - x, span(y, n), :] + more, 2, gq_r.at[1], gqk_r.at[1], across)

    gq_send(0, gqp[1 - x, span(1 - y, n), :], 0, d_r, dk_r, corner)

    @pl.when(c == 0)
    def _():
        gq_across(0.0)

    gq_send(1, gqp[x, span(1 - y, n), :], 1, gq_r.at[0], gqk_r.at[0], beside)

    half.wait_recv()

    for i in range(Z):
        k = turn(i)
        mine = dot(W[k], Q[1 - c], 0, 0)
        share(k).wait_recv()
        packed, step = pack(mine + dot(Ws[k], Qs[...], 0, 0))
        away = jnp.logical_or(z != k, crossed)

        @pl.when(away)
        def _():
            gpt[k], gpk[k] = packed, step
            remote(gpt.at[k], gpr.at[z], gp_s, gp_r, target(k)).start()
            remote(gpk.at[k], gpkr.at[z], gpk_s, gpk_r, target(k)).start()

        @pl.when(jnp.logical_not(away))
        def _():
            gpr[k], gpkr[k] = packed, step

    pltpu.make_async_copy(PM, PM, d_r).wait()
    pltpu.make_async_copy(gqk.at[0], gqk.at[0], dk_r).wait()

    @pl.when(c == 1)
    def _():
        gq_across(unpack(gqr, gqkr, 0))

    for j in (0, 1):
        pltpu.make_async_copy(PM, PM, gq_r.at[j]).wait()
        pltpu.make_async_copy(gqk.at[0], gqk.at[0], gqk_r.at[j]).wait()
    total = gqp[x, span(y, n), :] + unpack(gqr, gqkr, 1) + unpack(gqr, gqkr, 2)
    gq_ref[...] = total + unpack(gqr, gqkr, 0) * (1 - c).astype(F32)

    def gp_wait(count, data, step):
        pltpu.make_async_copy(gpr.at[pl.ds(0, count)], gpr.at[pl.ds(0, count)], data).wait()
        pltpu.make_async_copy(gpkr.at[pl.ds(0, count)], gpkr.at[pl.ds(0, count)], step).wait()

    def per_count(body):
        @pl.when(own)
        def _():
            body(Z - 1)

        @pl.when(crossed)
        def _():
            body(Z)

    per_count(lambda count: gp_wait(count, gp_r, gpk_r))
    gp_ref[...] = sum(unpack(gpr, gpkr, k) for k in range(Z))

    def p_wait(count):
        pltpu.make_async_copy(PB.at[0, pl.ds(0, count * n)], PB.at[0, pl.ds(0, count * n)], p_s).wait()
        gp_wait(count, gp_s, gpk_s)

    per_count(p_wait)
    for ref, sem in (
        (gqr, q_s),
        (PB.at[0], f_s),
        (W, w_s),
        (crc, c_s),
        (rrc, r_s),
        (gqt, gq_s),
        (gqk, gqk_s),
        (Qs, h_s),
    ):
        pltpu.make_async_copy(ref, ref, sem).wait()


def local(queries, passages, positives):
    n, w = queries.shape
    batch_count = lax.axis_size("batch")
    Z = batch_count // 4
    scale = 1.0 / math.sqrt(w * lax.axis_size("rep"))
    rows, cols = 2 * n, Z * n
    vmem = pl.BlockSpec(memory_space=pltpu.VMEM)
    dma = pltpu.SemaphoreType.DMA
    regular = pltpu.SemaphoreType.REGULAR
    hbm = pl.BlockSpec(memory_space=pltpu.HBM)
    operands = (queries, passages, positives.reshape(batch_count, n))
    grad_queries, grad_passages = pl.pallas_call(
        functools.partial(kernel, Z, scale),
        out_shape=(
            jax.ShapeDtypeStruct((n, w), F32),
            jax.ShapeDtypeStruct((n, w), F32),
        ),
        in_specs=[hbm] * 3,
        out_specs=(vmem, vmem),
        scratch_shapes=[
            pltpu.VMEM((2, rows, w), BF16),
            pltpu.VMEM((rows, w), BF16),
            pltpu.VMEM((2, cols, w), BF16),
            pltpu.VMEM((rows, cols), F32),
            pltpu.VMEM((Z, rows, n), F32),
            pltpu.VMEM((Z, rows, n), BF16),
            pltpu.VMEM((Z, rows, n), BF16),
            pltpu.VMEM((1, 2 * rows), F32),
            pltpu.VMEM((3, 1, 2 * rows), F32),
            pltpu.VMEM((1, 2 * cols), F32),
            pltpu.VMEM((2 * Z - 1, 1, 2 * cols), F32),
            pltpu.VMEM((n, w), BF16),
            pltpu.VMEM((batch_count, n), jnp.int32),
            pltpu.VMEM((2, rows, w), F32),
            pltpu.VMEM((3, n, w), I16),
            pltpu.VMEM((3, n, w), I16),
            pltpu.VMEM((3, 1, w), F32),
            pltpu.VMEM((3, 1, w), F32),
            pltpu.VMEM((Z, n, w), I16),
            pltpu.VMEM((Z, n, w), I16),
            pltpu.VMEM((Z, 1, w), F32),
            pltpu.VMEM((Z, 1, w), F32),
            regular((2,)),
            regular((Z,)),
            regular,
            dma((3,)),
            dma,
            dma((2,)),
            dma,
            dma((Z,)),
            dma,
            dma((Z,)),
            dma,
            dma,
            dma,
            dma,
            dma,
            dma,
            dma,
            dma((Z,)),
            dma,
            dma((2,)),
            dma,
            dma,
            dma,
            dma((2,)),
            dma,
            dma,
            dma,
            dma,
        ],
        compiler_params=pltpu.CompilerParams(collective_id=0, has_side_effects=True, vmem_limit_bytes=6 * 2**20 + 40 * rows * cols),
    )(*(pltpu.with_memory_space_constraint(a, pltpu.HBM) for a in operands))
    return grad_queries * scale, grad_passages * scale


def solution(mesh):
    in_specs = (P("batch", "rep"), P("batch", "rep"), P())
    out_specs = (P("batch", "rep"), P("batch", "rep"))
    return jax.shard_map(local, mesh=mesh, in_specs=in_specs, out_specs=out_specs, check_vma=False)
```

```python
import functools
import math

import jax
import jax.numpy as jnp
from jax import lax
from jax.experimental import pallas as pl
from jax.experimental.pallas import tpu as pltpu
from jax.sharding import PartitionSpec as P

MESH = pl.DeviceIdType.MESH
F32 = jnp.float32
BF16 = jnp.bfloat16
I16 = jnp.int16
TURNS = ((0, 1, 3, 2), (0, 3, 2, 1), (0, 3, 1, 2), (0, 2, 1, 3))


def dot(a, b, da, db):
    return lax.dot_general(a, b, (((da,), (db,)), ((), ())), preferred_element_type=F32)


def sent_bytes(n, w, Z, crossed=True):
    block, step = 2 * n * w, 4 * w
    blocks = 3 + (Z - 1 + crossed) + Z + 2 + 3 + (Z - 1 + crossed)
    steps = 3 + (Z - 1 + crossed)
    weights = Z * 2 * n * n * 2
    stats = (2 * Z - 1) * 2 * Z * n * 4 + 3 * 4 * n * 4
    return blocks * block + steps * step + weights + stats


def as_column(row, lanes):
    return jnp.broadcast_to(row, (lanes, row.shape[1])).T


def kernel(
    Z,
    scale,
    q_ref,
    p_ref,
    pos_hbm,
    gq_ref,
    gp_ref,
    Q,
    Qs,
    PB,
    S,
    A,
    W,
    Ws,
    rst,
    rrc,
    cst,
    crc,
    PM,
    pos_ref,
    span_ref,
    gqp,
    gqt,
    gqr,
    gqk,
    gqkr,
    gpt,
    gpr,
    gpk,
    gpkr,
    near,
    line,
    rest,
    in_s,
    out_s,
    q_r,
    p_r,
    f_r,
    h_r,
    r_r,
    c_r,
    w_r,
    gq_r,
    gp_r,
    d_r,
):
    n, w = q_ref.shape
    b = lax.axis_index("batch")
    x = lax.axis_index("rep")
    z, y, c = b // 4, (b // 2) % 2, b % 2
    rows, cols = 2 * n, Z * n

    def dev(zz, yy, cc, xx):
        return (zz * 4 + yy * 2 + cc, xx)

    def plane(j):
        xx = 1 - x if j & 1 else x
        yy = 1 - y if j & 2 else y
        return xx, yy

    def remote(src, dst, s, r, device):
        return pltpu.make_async_remote_copy(
            src_ref=src, dst_ref=dst, send_sem=s, recv_sem=r, device_id=device, device_id_type=MESH
        )

    def span(k, size):
        return pl.ds(k * size if isinstance(k, int) else pl.multiple_of(k * size, size), size)

    def settle(sem, size):
        ref = span_ref.at[:, pl.ds(0, size // 4)]
        pltpu.make_async_copy(ref, ref, sem).wait()

    packed_bytes = 2 * n * w + 4 * w

    def up(dz):
        return (z + dz) % Z

    own = c == 1 - x
    crossed = jnp.logical_not(own)
    sibling = dev(z, y, 1 - c, x)

    def target(zz):
        return dev(zz, y, 1 - x, 1 - c)

    barrier = pltpu.get_barrier_semaphore()

    q_own = Q.at[x, span(y, n)]
    p_in = pltpu.make_async_copy(p_ref, PM, in_s.at[0])
    q_in = pltpu.make_async_copy(q_ref, q_own, in_s.at[1])
    pos_in = pltpu.make_async_copy(pos_hbm, pos_ref, in_s.at[2])
    q_in.start()
    p_in.start()
    pos_in.start()

    def greet(sem, device):
        pl.semaphore_signal(sem, inc=1, device_id=device, device_id_type=MESH)

    place = 2 * y + x
    pairs = []
    for j in (1, 2):
        xx, yy = plane(j)
        pairs.append((2 * yy + xx < place, dev(z, yy, c, xx), near.at[j - 1]))
    pairs.append((c == 0, sibling, rest))
    for dz in range(1, Z):
        zz = up(dz)
        pairs.append((zz < z, target(zz), line.at[z]))
        for cc in (0, 1):
            pairs.append((zz < z, dev(zz, y, cc, x), rest))
    first = jnp.logical_and(crossed, x == 1)
    last = jnp.logical_and(crossed, x == 0)
    for earlier, device, _ in pairs:

        @pl.when(jnp.logical_not(earlier))
        def _():
            greet(barrier, device)

    @pl.when(last)
    def _():
        greet(barrier, target(z))

    greetings = x + y + 3 * z + (1 - c) + first.astype(jnp.int32)

    @pl.when(greetings > 0)
    def _():
        pl.semaphore_wait(barrier, greetings)

    for earlier, device, sem in pairs:

        @pl.when(earlier)
        def _():
            greet(sem, device)

    @pl.when(first)
    def _():
        greet(line.at[z], target(z))

    p_in.wait()
    p_block = PB.at[x, span(z, n)]

    def p_copy(zz):
        return remote(PM, p_block, out_s, p_r.at[z], target(zz))

    @pl.when(first)
    def _():
        p_copy(z).start()

    for k in range(Z - 1):

        @pl.when(k < z)
        def _():
            p_copy(k).start()

    q_in.wait()
    pos_in.wait()

    @pl.when(own)
    def _():
        PB[x, span(z, n), :] = PM[...]

    @pl.when(last)
    def _():
        pl.semaphore_wait(line.at[z], 1)
        p_copy(z).start()

    q_copies = []
    for j in (1, 2):
        xx, yy = plane(j)
        q_copies.append(remote(q_own, q_own, out_s, q_r.at[j - 1], dev(z, yy, c, xx)))

        @pl.when(2 * yy + xx > place)
        def _():
            pl.semaphore_wait(near.at[j - 1], 1)

        q_copies[-1].start()

    def send_later(zz):
        pl.semaphore_wait(line.at[zz], 1)
        p_copy(zz).start()

    @pl.when(jnp.logical_and(z > 0, z < Z - 1))
    def _():
        send_later(z + 1)

    for k in range(2, Z):

        @pl.when(k > z + 1)
        def _():
            send_later(k)

    @pl.when(z == 0)
    def _():
        send_later(1)

    answers = 2 * (Z - 1 - z) + c

    @pl.when(answers > 0)
    def _():
        pl.semaphore_wait(rest, answers)

    q_copies[0].wait_recv()
    q_far = Q.at[1 - x, span(y, n)]
    remote(q_far, q_far, out_s, q_r.at[1], dev(z, 1 - y, c, x)).start()

    def part(zz):
        return PB.at[1 - c, span(zz, n)]

    def forward(k):
        zz = nth(k)
        return remote(part(zz), part(zz), out_s, f_r.at[k // 2], sibling)

    def nth(k):
        return lax.select(k < Z - z, z + k, jnp.int32(Z - 1 - k))

    def scores(*ks):
        pltpu.make_async_copy(Q.at[0], Q.at[0], f_r.at[ks[0] // 2]).wait()
        parts = []
        for k in ks:
            zz = nth(k)
            at = span(zz, n)
            s = (dot(Q[0], PB[0, at, :], 1, 1) + dot(Q[1], PB[1, at, :], 1, 1)) * scale
            S[:, at] = s
            top = jnp.max(s, axis=0, keepdims=True)
            cst[:, at] = top
            cst[:, span(zz + Z, n)] = jnp.sum(jnp.exp(s - top), axis=0, keepdims=True)
            parts.append(s)
        return parts

    def row_part(parts, running):
        high = jnp.max(functools.reduce(jnp.maximum, parts), axis=1, keepdims=True)
        if running is not None:
            high = jnp.maximum(high, running[0])
        total = jnp.sum(sum(jnp.exp(s - high) for s in parts), axis=1, keepdims=True)
        if running is not None:
            total += running[1] * jnp.exp(running[0] - high)
        return high, total

    half = remote(Q.at[c], Qs, out_s, h_r, sibling)

    @pl.when(own)
    def _():
        forward(0).start()

    def arrive(k):
        zz = nth(k)

        @pl.when(jnp.logical_or(zz != z, crossed))
        def _():
            pltpu.make_async_copy(PM, part(zz), p_r.at[zz]).wait()
            forward(k).start()

    for k in range(Z):
        arrive(k)
    pltpu.make_async_copy(Q.at[0], Q.at[0], q_r.at[1]).wait()
    half.start()
    running = None
    for k in range(0, Z - 2, 2):
        running = row_part(scores(k, k + 1), running)
    parts = scores(Z - 2, Z - 1)

    col_copies = []
    for dz in range(Z):
        for dc in (0, 1):
            if dz or dc:
                k = dz * 2 + dc
                col_copies.append(
                    remote(cst, crc.at[k - 1], out_s, c_r, dev(up(dz), y, 1 - c if dc else c, x))
                )
                col_copies[-1].start()

    running = row_part(parts, running)

    def as_row(column):
        return jnp.broadcast_to(column, (rows, 128)).T[0:1, :]

    rst[:, 0:rows] = as_row(running[0])
    rst[:, rows : 2 * rows] = as_row(running[1])
    row_copies = []
    for j in (1, 2, 3):
        xx, yy = plane(j)
        row_copies.append(remote(rst, rrc.at[j - 1], out_s, r_r, dev(z, yy, c, xx)))
        row_copies[-1].start()

    places = jnp.concatenate(
        [
            as_column(pos_ref[pl.ds(z * 4 + yy * 2 + c, 1), :].astype(F32), 128)
            for yy in (0, 1)
        ],
        axis=0,
    )

    pltpu.make_async_copy(rrc, rrc, r_r).wait()
    high = rst[:, 0:rows]
    for j in range(3):
        high = jnp.maximum(high, rrc[j, :, 0:rows])
    total = rst[:, rows : 2 * rows] * jnp.exp(rst[:, 0:rows] - high)
    for j in range(3):
        total += rrc[j, :, rows : 2 * rows] * jnp.exp(rrc[j, :, 0:rows] - high)
    row_norm = as_column(high + jnp.log(total), 128)

    lane = lax.broadcasted_iota(jnp.int32, (rows, n), 1).astype(F32)
    for k in range(Z):
        base = lax.convert_element_type((k * 4 + y * 2 + 1 - x) * n, F32)
        hit = jnp.where(places - lane == base, 2.0, 0.0)
        A[k] = jnp.exp(S[:, span(k, n)] - row_norm) - hit

    pltpu.make_async_copy(crc, crc, c_r).wait()
    high = cst[:, 0:cols]
    for k in range(2 * Z - 1):
        high = jnp.maximum(high, crc[k, :, 0:cols])
    total = cst[:, cols : 2 * cols] * jnp.exp(cst[:, 0:cols] - high)
    for k in range(2 * Z - 1):
        total += crc[k, :, cols : 2 * cols] * jnp.exp(crc[k, :, 0:cols] - high)
    crc[0, :, 0:cols] = high + jnp.log(total)

    def turn(i):
        if Z != 4:
            return jnp.int32(i)
        first_z, second_z, third_z, fourth_z = (row[i] for row in TURNS)
        low = lax.select(z == 0, jnp.int32(first_z), jnp.int32(second_z))
        high = lax.select(z == 2, jnp.int32(third_z), jnp.int32(fourth_z))
        return lax.select(z < 2, low, high)

    def share(k):
        return remote(W.at[k], Ws.at[k], out_s, w_r.at[k], sibling)

    for i in range(Z):
        k = turn(i)
        W[k] = (A[k] + jnp.exp(S[:, span(k, n)] - crc[0, :, span(k, n)])).astype(BF16)
        share(k).start()

    def pack(value):
        top = jnp.maximum(jnp.max(jnp.abs(value), axis=0, keepdims=True), 1e-30)
        return jnp.round(value * (32766.0 / top)).astype(jnp.int32).astype(I16), top * (1.0 / 32766.0)

    def unpack(at, step, k):
        return at[k].astype(jnp.int32).astype(F32) * step[k]

    def query_terms(h):
        def term(k):
            return dot(W[k], PB[h, span(k, n), :], 1, 0)

        if Z <= 4:
            return dot(jnp.concatenate([W[k] for k in range(Z)], axis=1), PB[h], 1, 0)
        return lax.fori_loop(0, Z, lambda k, t: t + term(k), jnp.zeros((rows, w), F32))

    def gq_send(j, value, slot, data, step, device):
        gqt[j], gqk[j] = pack(value)
        remote(gqt.at[j], gqr.at[slot], out_s, data, device).start()
        remote(gqk.at[j], gqkr.at[slot], out_s, step, device).start()

    for h in (0, 1):
        gqp[h] = query_terms(h)
    beside, across = dev(z, 1 - y, c, x), dev(z, y, c, 1 - x)
    corner = dev(z, 1 - y, c, lax.select(c == 1, x, 1 - x))

    def gq_across(more):
        gq_send(2, gqp[1 - x, span(y, n), :] + more, 2, gq_r.at[1], gq_r.at[1], across)

    gq_send(0, gqp[1 - x, span(1 - y, n), :], 0, d_r, d_r, corner)

    @pl.when(c == 0)
    def _():
        gq_across(0.0)

    gq_send(1, gqp[x, span(1 - y, n), :], 1, gq_r.at[0], gq_r.at[0], beside)

    half.wait_recv()

    for i in range(Z):
        k = turn(i)
        mine = dot(W[k], Q[1 - c], 0, 0)
        share(k).wait_recv()
        packed, step = pack(mine + dot(Ws[k], Qs[...], 0, 0))
        away = jnp.logical_or(z != k, crossed)

        @pl.when(away)
        def _():
            gpt[k], gpk[k] = packed, step
            remote(gpt.at[k], gpr.at[z], out_s, gp_r, target(k)).start()
            remote(gpk.at[k], gpkr.at[z], out_s, gp_r, target(k)).start()

        @pl.when(jnp.logical_not(away))
        def _():
            gpr[k], gpkr[k] = packed, step

    settle(d_r, packed_bytes)

    @pl.when(c == 1)
    def _():
        gq_across(unpack(gqr, gqkr, 0))

    for j in (0, 1):
        settle(gq_r.at[j], packed_bytes)
    total = gqp[x, span(y, n), :] + unpack(gqr, gqkr, 1) + unpack(gqr, gqkr, 2)
    gq_ref[...] = total + unpack(gqr, gqkr, 0) * (1 - c).astype(F32)

    def per_count(body):
        @pl.when(own)
        def _():
            body(Z - 1)

        @pl.when(crossed)
        def _():
            body(Z)

    per_count(lambda count: settle(gp_r, count * packed_bytes))
    gp_ref[...] = sum(unpack(gpr, gpkr, k) for k in range(Z))

    per_count(lambda count: settle(out_s, sent_bytes(n, w, Z, count == Z)))


def local(queries, passages, positives):
    n, w = queries.shape
    batch_count = lax.axis_size("batch")
    Z = batch_count // 4
    scale = 1.0 / math.sqrt(w * lax.axis_size("rep"))
    rows, cols = 2 * n, Z * n
    vmem = pl.BlockSpec(memory_space=pltpu.VMEM)
    dma = pltpu.SemaphoreType.DMA
    regular = pltpu.SemaphoreType.REGULAR
    hbm = pl.BlockSpec(memory_space=pltpu.HBM)
    operands = (queries, passages, positives.reshape(batch_count, n))
    grad_queries, grad_passages = pl.pallas_call(
        functools.partial(kernel, Z, scale),
        out_shape=(
            jax.ShapeDtypeStruct((n, w), F32),
            jax.ShapeDtypeStruct((n, w), F32),
        ),
        in_specs=[hbm] * 3,
        out_specs=(vmem, vmem),
        scratch_shapes=[
            pltpu.VMEM((2, rows, w), BF16),
            pltpu.VMEM((rows, w), BF16),
            pltpu.VMEM((2, cols, w), BF16),
            pltpu.VMEM((rows, cols), F32),
            pltpu.VMEM((Z, rows, n), F32),
            pltpu.VMEM((Z, rows, n), BF16),
            pltpu.VMEM((Z, rows, n), BF16),
            pltpu.VMEM((1, 2 * rows), F32),
            pltpu.VMEM((3, 1, 2 * rows), F32),
            pltpu.VMEM((1, 2 * cols), F32),
            pltpu.VMEM((2 * Z - 1, 1, 2 * cols), F32),
            pltpu.VMEM((n, w), BF16),
            pltpu.VMEM((batch_count, n), jnp.int32),
            pltpu.VMEM((1, sent_bytes(n, w, Z) // 4), F32),
            pltpu.VMEM((2, rows, w), F32),
            pltpu.VMEM((3, n, w), I16),
            pltpu.VMEM((3, n, w), I16),
            pltpu.VMEM((3, 1, w), F32),
            pltpu.VMEM((3, 1, w), F32),
            pltpu.VMEM((Z, n, w), I16),
            pltpu.VMEM((Z, n, w), I16),
            pltpu.VMEM((Z, 1, w), F32),
            pltpu.VMEM((Z, 1, w), F32),
            regular((2,)),
            regular((Z,)),
            regular,
            dma((3,)),
            dma,
            dma((2,)),
            dma((Z,)),
            dma((Z // 2,)),
            dma,
            dma,
            dma,
            dma((Z,)),
            dma((2,)),
            dma,
            dma,
        ],
        compiler_params=pltpu.CompilerParams(collective_id=0, has_side_effects=True, vmem_limit_bytes=6 * 2**20 + 40 * rows * cols),
    )(*(pltpu.with_memory_space_constraint(a, pltpu.HBM) for a in operands))
    return grad_queries * scale, grad_passages * scale


def solution(mesh):
    in_specs = (P("batch", "rep"), P("batch", "rep"), P())
    out_specs = (P("batch", "rep"), P("batch", "rep"))
    return jax.shard_map(local, mesh=mesh, in_specs=in_specs, out_specs=out_specs, check_vma=False)
```

```python
import functools
import math

import jax
import jax.numpy as jnp
from jax import lax
from jax.experimental import pallas as pl
from jax.experimental.pallas import tpu as pltpu
from jax.sharding import PartitionSpec as P

MESH = pl.DeviceIdType.MESH
F32 = jnp.float32
BF16 = jnp.bfloat16
I16 = jnp.int16
TURNS = ((0, 1, 3, 2), (0, 3, 2, 1), (0, 3, 1, 2), (2, 0, 1, 3))


def dot(a, b, da, db):
    return lax.dot_general(a, b, (((da,), (db,)), ((), ())), preferred_element_type=F32)


def sent_bytes(n, w, Z, crossed=True):
    block, step = 2 * n * w, 4 * w
    blocks = 3 + (Z - 1 + crossed) + Z + 2 + 3 + (Z - 1 + crossed)
    steps = 3 + (Z - 1 + crossed)
    weights = Z * 2 * n * n * 2
    stats = (2 * Z - 1) * 2 * Z * n * 4 + 3 * 4 * n * 4
    return blocks * block + steps * step + weights + stats


def as_column(row, lanes):
    return jnp.broadcast_to(row, (lanes, row.shape[1])).T


def kernel(
    Z,
    scale,
    q_ref,
    p_ref,
    pos_hbm,
    gq_ref,
    gp_ref,
    Q,
    Qs,
    PB,
    S,
    A,
    W,
    Ws,
    rst,
    rrc,
    cst,
    crc,
    PM,
    pos_ref,
    span_ref,
    gqp,
    gqt,
    gqr,
    gqk,
    gqkr,
    gpt,
    gpr,
    gpk,
    gpkr,
    near,
    line,
    rest,
    in_s,
    out_s,
    q_r,
    p_r,
    f_r,
    h_r,
    r_r,
    c_r,
    w_r,
    gq_r,
    gp_r,
    d_r,
):
    n, w = q_ref.shape
    b = lax.axis_index("batch")
    x = lax.axis_index("rep")
    z, y, c = b // 4, (b // 2) % 2, b % 2
    rows, cols = 2 * n, Z * n

    def dev(zz, yy, cc, xx):
        return (zz * 4 + yy * 2 + cc, xx)

    def plane(j):
        xx = 1 - x if j & 1 else x
        yy = 1 - y if j & 2 else y
        return xx, yy

    def remote(src, dst, s, r, device):
        return pltpu.make_async_remote_copy(
            src_ref=src, dst_ref=dst, send_sem=s, recv_sem=r, device_id=device, device_id_type=MESH
        )

    def span(k, size):
        return pl.ds(k * size if isinstance(k, int) else pl.multiple_of(k * size, size), size)

    def settle(sem, size):
        ref = span_ref.at[:, pl.ds(0, size // 4)]
        pltpu.make_async_copy(ref, ref, sem).wait()

    packed_bytes = 2 * n * w + 4 * w

    def up(dz):
        return (z + dz) % Z

    own = c == 1 - x
    crossed = jnp.logical_not(own)
    sibling = dev(z, y, 1 - c, x)

    def target(zz):
        return dev(zz, y, 1 - x, 1 - c)

    barrier = pltpu.get_barrier_semaphore()

    q_own = Q.at[x, span(y, n)]
    p_in = pltpu.make_async_copy(p_ref, PM, in_s.at[0])
    q_in = pltpu.make_async_copy(q_ref, q_own, in_s.at[1])
    pos_in = pltpu.make_async_copy(pos_hbm, pos_ref, in_s.at[2])
    q_in.start()
    p_in.start()
    pos_in.start()

    def greet(sem, device):
        pl.semaphore_signal(sem, inc=1, device_id=device, device_id_type=MESH)

    place = 2 * y + x
    pairs = []
    for j in (1, 2):
        xx, yy = plane(j)
        pairs.append((2 * yy + xx < place, dev(z, yy, c, xx), near.at[j - 1]))
    pairs.append((c == 0, sibling, rest))
    for dz in range(1, Z):
        zz = up(dz)
        pairs.append((zz < z, target(zz), line.at[z]))
        for cc in (0, 1):
            pairs.append((zz < z, dev(zz, y, cc, x), rest))
    first = jnp.logical_and(crossed, x == 1)
    last = jnp.logical_and(crossed, x == 0)
    for earlier, device, _ in pairs:

        @pl.when(jnp.logical_not(earlier))
        def _():
            greet(barrier, device)

    @pl.when(last)
    def _():
        greet(barrier, target(z))

    greetings = x + y + 3 * z + (1 - c) + first.astype(jnp.int32)

    @pl.when(greetings > 0)
    def _():
        pl.semaphore_wait(barrier, greetings)

    for earlier, device, sem in pairs:

        @pl.when(earlier)
        def _():
            greet(sem, device)

    @pl.when(first)
    def _():
        greet(line.at[z], target(z))

    p_in.wait()
    p_block = PB.at[x, span(z, n)]

    def p_copy(zz):
        return remote(PM, p_block, out_s, p_r.at[z], target(zz))

    @pl.when(first)
    def _():
        p_copy(z).start()

    for k in range(Z - 1):

        @pl.when(k < z)
        def _():
            p_copy(k).start()

    q_in.wait()
    pos_in.wait()

    @pl.when(own)
    def _():
        PB[x, span(z, n), :] = PM[...]

    @pl.when(last)
    def _():
        pl.semaphore_wait(line.at[z], 1)
        p_copy(z).start()

    q_copies = []
    for j in (1, 2):
        xx, yy = plane(j)
        q_copies.append(remote(q_own, q_own, out_s, q_r.at[j - 1], dev(z, yy, c, xx)))

        @pl.when(2 * yy + xx > place)
        def _():
            pl.semaphore_wait(near.at[j - 1], 1)

        q_copies[-1].start()

    def send_later(zz):
        pl.semaphore_wait(line.at[zz], 1)
        p_copy(zz).start()

    @pl.when(z < Z - 1)
    def _():
        send_later(z + 1)

    for k in range(2, Z):

        @pl.when(k > z + 1)
        def _():
            send_later(k)

    answers = 2 * (Z - 1 - z) + c

    @pl.when(answers > 0)
    def _():
        pl.semaphore_wait(rest, answers)

    q_copies[0].wait_recv()
    q_far = Q.at[1 - x, span(y, n)]
    remote(q_far, q_far, out_s, q_r.at[1], dev(z, 1 - y, c, x)).start()

    def part(zz):
        return PB.at[1 - c, span(zz, n)]

    def forward(k):
        zz = nth(k)
        return remote(part(zz), part(zz), out_s, f_r.at[k // 2], sibling)

    def nth(k):
        return lax.select(k < Z - z, z + k, jnp.int32(Z - 1 - k))

    def scores(*ks):
        pltpu.make_async_copy(Q.at[0], Q.at[0], f_r.at[ks[0] // 2]).wait()
        parts = []
        for k in ks:
            zz = nth(k)
            at = span(zz, n)
            s = (dot(Q[0], PB[0, at, :], 1, 1) + dot(Q[1], PB[1, at, :], 1, 1)) * scale
            S[:, at] = s
            top = jnp.max(s, axis=0, keepdims=True)
            cst[:, at] = top
            cst[:, span(zz + Z, n)] = jnp.sum(jnp.exp(s - top), axis=0, keepdims=True)
            parts.append(s)
        return parts

    def row_part(parts, running):
        high = jnp.max(functools.reduce(jnp.maximum, parts), axis=1, keepdims=True)
        if running is not None:
            high = jnp.maximum(high, running[0])
        total = jnp.sum(sum(jnp.exp(s - high) for s in parts), axis=1, keepdims=True)
        if running is not None:
            total += running[1] * jnp.exp(running[0] - high)
        return high, total

    half = remote(Q.at[c], Qs, out_s, h_r, sibling)

    @pl.when(own)
    def _():
        forward(0).start()

    def arrive(k):
        zz = nth(k)

        @pl.when(jnp.logical_or(zz != z, crossed))
        def _():
            pltpu.make_async_copy(PM, part(zz), p_r.at[zz]).wait()
            forward(k).start()

    for k in range(Z):
        arrive(k)
    pltpu.make_async_copy(Q.at[0], Q.at[0], q_r.at[1]).wait()
    half.start()
    running = None
    for k in range(0, Z - 2, 2):
        running = row_part(scores(k, k + 1), running)
    parts = scores(Z - 2, Z - 1)

    col_copies = []
    for dz in range(Z):
        for dc in (0, 1):
            if dz or dc:
                k = dz * 2 + dc
                col_copies.append(
                    remote(cst, crc.at[k - 1], out_s, c_r, dev(up(dz), y, 1 - c if dc else c, x))
                )
                col_copies[-1].start()

    running = row_part(parts, running)

    def as_row(column):
        return jnp.broadcast_to(column, (rows, 128)).T[0:1, :]

    rst[:, 0:rows] = as_row(running[0])
    rst[:, rows : 2 * rows] = as_row(running[1])
    row_copies = []
    for j in (1, 2, 3):
        xx, yy = plane(j)
        row_copies.append(remote(rst, rrc.at[j - 1], out_s, r_r, dev(z, yy, c, xx)))
        row_copies[-1].start()

    places = jnp.concatenate(
        [
            as_column(pos_ref[pl.ds(z * 4 + yy * 2 + c, 1), :].astype(F32), 128)
            for yy in (0, 1)
        ],
        axis=0,
    )

    pltpu.make_async_copy(rrc, rrc, r_r).wait()
    high = rst[:, 0:rows]
    for j in range(3):
        high = jnp.maximum(high, rrc[j, :, 0:rows])
    total = rst[:, rows : 2 * rows] * jnp.exp(rst[:, 0:rows] - high)
    for j in range(3):
        total += rrc[j, :, rows : 2 * rows] * jnp.exp(rrc[j, :, 0:rows] - high)
    row_norm = as_column(high + jnp.log(total), 128)

    lane = lax.broadcasted_iota(jnp.int32, (rows, n), 1).astype(F32)
    for k in range(Z):
        base = lax.convert_element_type((k * 4 + y * 2 + 1 - x) * n, F32)
        hit = jnp.where(places - lane == base, 2.0, 0.0)
        A[k] = jnp.exp(S[:, span(k, n)] - row_norm) - hit

    pltpu.make_async_copy(crc, crc, c_r).wait()
    high = cst[:, 0:cols]
    for k in range(2 * Z - 1):
        high = jnp.maximum(high, crc[k, :, 0:cols])
    total = cst[:, cols : 2 * cols] * jnp.exp(cst[:, 0:cols] - high)
    for k in range(2 * Z - 1):
        total += crc[k, :, cols : 2 * cols] * jnp.exp(crc[k, :, 0:cols] - high)
    crc[0, :, 0:cols] = high + jnp.log(total)

    def turn(i):
        if Z != 4:
            return jnp.int32(i)
        first_z, second_z, third_z, fourth_z = (row[i] for row in TURNS)
        low = lax.select(z == 0, jnp.int32(first_z), jnp.int32(second_z))
        high = lax.select(z == 2, jnp.int32(third_z), jnp.int32(fourth_z))
        return lax.select(z < 2, low, high)

    def share(k):
        return remote(W.at[k], Ws.at[k], out_s, w_r.at[k], sibling)

    for i in range(Z):
        k = turn(i)
        W[k] = (A[k] + jnp.exp(S[:, span(k, n)] - crc[0, :, span(k, n)])).astype(BF16)
        share(k).start()

    def pack(value):
        top = jnp.maximum(jnp.max(jnp.abs(value), axis=0, keepdims=True), 1e-30)
        return jnp.round(value * (32766.0 / top)).astype(jnp.int32).astype(I16), top * (1.0 / 32766.0)

    def unpack(at, step, k):
        return at[k].astype(jnp.int32).astype(F32) * step[k]

    def query_terms(h):
        def term(k):
            return dot(W[k], PB[h, span(k, n), :], 1, 0)

        if Z <= 4:
            return dot(jnp.concatenate([W[k] for k in range(Z)], axis=1), PB[h], 1, 0)
        return lax.fori_loop(0, Z, lambda k, t: t + term(k), jnp.zeros((rows, w), F32))

    def gq_send(j, value, slot, data, step, device):
        gqt[j], gqk[j] = pack(value)
        remote(gqt.at[j], gqr.at[slot], out_s, data, device).start()
        remote(gqk.at[j], gqkr.at[slot], out_s, step, device).start()

    for h in (0, 1):
        gqp[h] = query_terms(h)
    beside, across = dev(z, 1 - y, c, x), dev(z, y, c, 1 - x)
    corner = dev(z, 1 - y, c, lax.select(c == 1, x, 1 - x))

    def gq_across(more):
        gq_send(2, gqp[1 - x, span(y, n), :] + more, 2, gq_r.at[1], gq_r.at[1], across)

    gq_send(0, gqp[1 - x, span(1 - y, n), :], 0, d_r, d_r, corner)

    @pl.when(c == 0)
    def _():
        gq_across(0.0)

    gq_send(1, gqp[x, span(1 - y, n), :], 1, gq_r.at[0], gq_r.at[0], beside)

    half.wait_recv()

    for i in range(Z):
        k = turn(i)
        mine = dot(W[k], Q[1 - c], 0, 0)
        share(k).wait_recv()
        packed, step = pack(mine + dot(Ws[k], Qs[...], 0, 0))
        away = jnp.logical_or(z != k, crossed)

        @pl.when(away)
        def _():
            gpt[k], gpk[k] = packed, step
            remote(gpt.at[k], gpr.at[z], out_s, gp_r, target(k)).start()
            remote(gpk.at[k], gpkr.at[z], out_s, gp_r, target(k)).start()

        @pl.when(jnp.logical_not(away))
        def _():
            gpr[k], gpkr[k] = packed, step

    settle(d_r, packed_bytes)

    @pl.when(c == 1)
    def _():
        gq_across(unpack(gqr, gqkr, 0))

    for j in (0, 1):
        settle(gq_r.at[j], packed_bytes)
    total = gqp[x, span(y, n), :] + unpack(gqr, gqkr, 1) + unpack(gqr, gqkr, 2)
    gq_ref[...] = total + unpack(gqr, gqkr, 0) * (1 - c).astype(F32)

    def per_count(body):
        @pl.when(own)
        def _():
            body(Z - 1)

        @pl.when(crossed)
        def _():
            body(Z)

    per_count(lambda count: settle(gp_r, count * packed_bytes))
    gp_ref[...] = sum(unpack(gpr, gpkr, k) for k in range(Z))

    per_count(lambda count: settle(out_s, sent_bytes(n, w, Z, count == Z)))


def local(queries, passages, positives):
    n, w = queries.shape
    batch_count = lax.axis_size("batch")
    Z = batch_count // 4
    scale = 1.0 / math.sqrt(w * lax.axis_size("rep"))
    rows, cols = 2 * n, Z * n
    vmem = pl.BlockSpec(memory_space=pltpu.VMEM)
    dma = pltpu.SemaphoreType.DMA
    regular = pltpu.SemaphoreType.REGULAR
    hbm = pl.BlockSpec(memory_space=pltpu.HBM)
    operands = (queries, passages, positives.reshape(batch_count, n))
    grad_queries, grad_passages = pl.pallas_call(
        functools.partial(kernel, Z, scale),
        out_shape=(
            jax.ShapeDtypeStruct((n, w), F32),
            jax.ShapeDtypeStruct((n, w), F32),
        ),
        in_specs=[hbm] * 3,
        out_specs=(vmem, vmem),
        scratch_shapes=[
            pltpu.VMEM((2, rows, w), BF16),
            pltpu.VMEM((rows, w), BF16),
            pltpu.VMEM((2, cols, w), BF16),
            pltpu.VMEM((rows, cols), F32),
            pltpu.VMEM((Z, rows, n), F32),
            pltpu.VMEM((Z, rows, n), BF16),
            pltpu.VMEM((Z, rows, n), BF16),
            pltpu.VMEM((1, 2 * rows), F32),
            pltpu.VMEM((3, 1, 2 * rows), F32),
            pltpu.VMEM((1, 2 * cols), F32),
            pltpu.VMEM((2 * Z - 1, 1, 2 * cols), F32),
            pltpu.VMEM((n, w), BF16),
            pltpu.VMEM((batch_count, n), jnp.int32),
            pltpu.VMEM((1, sent_bytes(n, w, Z) // 4), F32),
            pltpu.VMEM((2, rows, w), F32),
            pltpu.VMEM((3, n, w), I16),
            pltpu.VMEM((3, n, w), I16),
            pltpu.VMEM((3, 1, w), F32),
            pltpu.VMEM((3, 1, w), F32),
            pltpu.VMEM((Z, n, w), I16),
            pltpu.VMEM((Z, n, w), I16),
            pltpu.VMEM((Z, 1, w), F32),
            pltpu.VMEM((Z, 1, w), F32),
            regular((2,)),
            regular((Z,)),
            regular,
            dma((3,)),
            dma,
            dma((2,)),
            dma((Z,)),
            dma((Z // 2,)),
            dma,
            dma,
            dma,
            dma((Z,)),
            dma((2,)),
            dma,
            dma,
        ],
        compiler_params=pltpu.CompilerParams(collective_id=0, has_side_effects=True, vmem_limit_bytes=6 * 2**20 + 40 * rows * cols),
    )(*(pltpu.with_memory_space_constraint(a, pltpu.HBM) for a in operands))
    return grad_queries * scale, grad_passages * scale


def solution(mesh):
    in_specs = (P("batch", "rep"), P("batch", "rep"), P())
    out_specs = (P("batch", "rep"), P("batch", "rep"))
    return jax.shard_map(local, mesh=mesh, in_specs=in_specs, out_specs=out_specs, check_vma=False)
```

```python
import functools
import math

import jax
import jax.numpy as jnp
from jax import lax
from jax.experimental import pallas as pl
from jax.experimental.pallas import tpu as pltpu
from jax.sharding import PartitionSpec as P

MESH = pl.DeviceIdType.MESH
F32 = jnp.float32
BF16 = jnp.bfloat16
I16 = jnp.int16
TURNS = ((0, 1, 3, 2), (0, 3, 2, 1), (0, 3, 1, 2), (2, 0, 1, 3))


def dot(a, b, da, db):
    return lax.dot_general(a, b, (((da,), (db,)), ((), ())), preferred_element_type=F32)


def sent_bytes(n, w, Z, crossed=True):
    block, step = 2 * n * w, 4 * w
    blocks = 3 + (Z - 1 + crossed) + Z + 2 + 3 + (Z - 1 + crossed)
    steps = 3 + (Z - 1 + crossed)
    weights = Z * 2 * n * n * 2
    stats = (2 * Z - 1) * 2 * Z * n * 4 + 3 * 4 * n * 4
    return blocks * block + steps * step + weights + stats


def as_column(row, lanes):
    return jnp.broadcast_to(row, (lanes, row.shape[1])).T


def kernel(
    Z,
    scale,
    q_ref,
    p_ref,
    pos_hbm,
    gq_ref,
    gp_ref,
    Q,
    Qs,
    PB,
    S,
    A,
    W,
    Ws,
    rst,
    rrc,
    cst,
    crc,
    PM,
    pos_ref,
    span_ref,
    gqp,
    gqt,
    gqr,
    gqk,
    gqkr,
    gpt,
    gpr,
    gpk,
    gpkr,
    near,
    line,
    rest,
    in_s,
    out_s,
    q_r,
    p_r,
    f_r,
    r_r,
    c_r,
    w_r,
    gq_r,
    gp_r,
    d_r,
):
    n, w = q_ref.shape
    b = lax.axis_index("batch")
    x = lax.axis_index("rep")
    z, y, c = b // 4, (b // 2) % 2, b % 2
    rows, cols = 2 * n, Z * n

    def dev(zz, yy, cc, xx):
        return (zz * 4 + yy * 2 + cc, xx)

    def plane(j):
        xx = 1 - x if j & 1 else x
        yy = 1 - y if j & 2 else y
        return xx, yy

    def remote(src, dst, s, r, device):
        return pltpu.make_async_remote_copy(
            src_ref=src, dst_ref=dst, send_sem=s, recv_sem=r, device_id=device, device_id_type=MESH
        )

    def span(k, size):
        return pl.ds(k * size if isinstance(k, int) else pl.multiple_of(k * size, size), size)

    def settle(sem, size):
        ref = span_ref.at[:, pl.ds(0, size // 4)]
        pltpu.make_async_copy(ref, ref, sem).wait()

    packed_bytes = 2 * n * w + 4 * w

    def up(dz):
        return (z + dz) % Z

    own = c == 1 - x
    crossed = jnp.logical_not(own)
    sibling = dev(z, y, 1 - c, x)

    def target(zz):
        return dev(zz, y, 1 - x, 1 - c)

    barrier = pltpu.get_barrier_semaphore()

    q_own = Q.at[x, span(y, n)]
    p_in = pltpu.make_async_copy(p_ref, PM, in_s)
    q_in = pltpu.make_async_copy(q_ref, q_own, in_s)
    pos_in = pltpu.make_async_copy(pos_hbm, pos_ref, in_s)
    q_in.start()
    p_in.start()
    pos_in.start()

    def greet(sem, device):
        pl.semaphore_signal(sem, inc=1, device_id=device, device_id_type=MESH)

    place = 2 * y + x
    pairs = []
    for j in (1, 2):
        xx, yy = plane(j)
        pairs.append((2 * yy + xx < place, dev(z, yy, c, xx), near.at[j - 1]))
    pairs.append((c == 0, sibling, rest))
    for dz in range(1, Z):
        zz = up(dz)
        pairs.append((zz < z, target(zz), line.at[z]))
        for cc in (0, 1):
            pairs.append((zz < z, dev(zz, y, cc, x), rest))
    first = jnp.logical_and(crossed, x == 1)
    last = jnp.logical_and(crossed, x == 0)
    for earlier, device, _ in pairs:

        @pl.when(jnp.logical_not(earlier))
        def _():
            greet(barrier, device)

    @pl.when(last)
    def _():
        greet(barrier, target(z))

    greetings = x + y + 3 * z + (1 - c) + first.astype(jnp.int32)

    @pl.when(greetings > 0)
    def _():
        pl.semaphore_wait(barrier, greetings)

    for earlier, device, sem in pairs:

        @pl.when(earlier)
        def _():
            greet(sem, device)

    @pl.when(first)
    def _():
        greet(line.at[z], target(z))

    settle(in_s, 4 * n * w + 4 * pos_ref.shape[0] * n)
    p_block = PB.at[x, span(z, n)]

    def p_copy(zz):
        return remote(PM, p_block, out_s, p_r.at[z], target(zz))

    @pl.when(first)
    def _():
        p_copy(z).start()

    for k in range(Z - 1):

        @pl.when(k < z)
        def _():
            p_copy(k).start()

    @pl.when(own)
    def _():
        PB[x, span(z, n), :] = PM[...]

    @pl.when(last)
    def _():
        pl.semaphore_wait(line.at[z], 1)
        p_copy(z).start()

    q_copies = []
    for j in (1, 2):
        xx, yy = plane(j)
        q_copies.append(remote(q_own, q_own, out_s, q_r.at[j - 1], dev(z, yy, c, xx)))

        @pl.when(2 * yy + xx > place)
        def _():
            pl.semaphore_wait(near.at[j - 1], 1)

        q_copies[-1].start()

    def send_later(zz):
        pl.semaphore_wait(line.at[zz], 1)
        p_copy(zz).start()

    nearest_last = jnp.logical_and(z > 0, jnp.logical_and(c == 0, x == 1))

    @pl.when(jnp.logical_and(z < Z - 1, jnp.logical_not(nearest_last)))
    def _():
        send_later(z + 1)

    for k in range(2, Z):

        @pl.when(k > z + 1)
        def _():
            send_later(k)

    @pl.when(jnp.logical_and(z < Z - 1, nearest_last))
    def _():
        send_later(z + 1)

    answers = 2 * (Z - 1 - z) + c

    @pl.when(answers > 0)
    def _():
        pl.semaphore_wait(rest, answers)

    q_copies[0].wait_recv()
    q_far = Q.at[1 - x, span(y, n)]
    remote(q_far, q_far, out_s, q_r.at[1], dev(z, 1 - y, c, x)).start()

    def part(zz):
        return PB.at[1 - c, span(zz, n)]

    def forward(k):
        zz = nth(k)
        return remote(part(zz), part(zz), out_s, f_r.at[k // 2], sibling)

    def nth(k):
        return lax.select(k < Z - z, z + k, jnp.int32(Z - 1 - k))

    def scores(*ks):
        pltpu.make_async_copy(Q.at[0], Q.at[0], f_r.at[ks[0] // 2]).wait()
        parts = []
        for k in ks:
            zz = nth(k)
            at = span(zz, n)
            s = (dot(Q[0], PB[0, at, :], 1, 1) + dot(Q[1], PB[1, at, :], 1, 1)) * scale
            S[:, at] = s
            top = jnp.max(s, axis=0, keepdims=True)
            cst[:, at] = top
            cst[:, span(zz + Z, n)] = jnp.sum(jnp.exp(s - top), axis=0, keepdims=True)
            parts.append(s)
        return parts

    def row_part(parts, running):
        high = jnp.max(functools.reduce(jnp.maximum, parts), axis=1, keepdims=True)
        if running is not None:
            high = jnp.maximum(high, running[0])
        total = jnp.sum(sum(jnp.exp(s - high) for s in parts), axis=1, keepdims=True)
        if running is not None:
            total += running[1] * jnp.exp(running[0] - high)
        return high, total

    half = remote(Q.at[c], Qs, out_s, w_r.at[0], sibling)

    @pl.when(own)
    def _():
        forward(0).start()

    def arrive(k):
        zz = nth(k)

        @pl.when(jnp.logical_or(zz != z, crossed))
        def _():
            pltpu.make_async_copy(PM, part(zz), p_r.at[zz]).wait()
            forward(k).start()

    for k in range(Z):
        arrive(k)
    pltpu.make_async_copy(Q.at[0], Q.at[0], q_r.at[1]).wait()
    half.start()
    running = None
    for k in range(0, Z - 2, 2):
        running = row_part(scores(k, k + 1), running)
    parts = scores(Z - 2, Z - 1)

    col_copies = []
    for dz in range(Z):
        for dc in (0, 1):
            if dz or dc:
                k = dz * 2 + dc
                col_copies.append(
                    remote(cst, crc.at[k - 1], out_s, c_r, dev(up(dz), y, 1 - c if dc else c, x))
                )
                col_copies[-1].start()

    running = row_part(parts, running)

    def as_row(column):
        return jnp.broadcast_to(column, (rows, 128)).T[0:1, :]

    rst[:, 0:rows] = as_row(running[0])
    rst[:, rows : 2 * rows] = as_row(running[1])
    row_copies = []
    for j in (1, 2, 3):
        xx, yy = plane(j)
        row_copies.append(remote(rst, rrc.at[j - 1], out_s, r_r, dev(z, yy, c, xx)))
        row_copies[-1].start()

    places = jnp.concatenate(
        [
            as_column(pos_ref[pl.ds(z * 4 + yy * 2 + c, 1), :].astype(F32), 128)
            for yy in (0, 1)
        ],
        axis=0,
    )

    pltpu.make_async_copy(rrc, rrc, r_r).wait()
    high = rst[:, 0:rows]
    for j in range(3):
        high = jnp.maximum(high, rrc[j, :, 0:rows])
    total = rst[:, rows : 2 * rows] * jnp.exp(rst[:, 0:rows] - high)
    for j in range(3):
        total += rrc[j, :, rows : 2 * rows] * jnp.exp(rrc[j, :, 0:rows] - high)
    row_norm = as_column(high + jnp.log(total), 128)

    lane = lax.broadcasted_iota(jnp.int32, (rows, n), 1).astype(F32)
    for k in range(Z):
        base = lax.convert_element_type((k * 4 + y * 2 + 1 - x) * n, F32)
        hit = jnp.where(places - lane == base, 2.0, 0.0)
        A[k] = jnp.exp(S[:, span(k, n)] - row_norm) - hit

    pltpu.make_async_copy(crc, crc, c_r).wait()
    high = cst[:, 0:cols]
    for k in range(2 * Z - 1):
        high = jnp.maximum(high, crc[k, :, 0:cols])
    total = cst[:, cols : 2 * cols] * jnp.exp(cst[:, 0:cols] - high)
    for k in range(2 * Z - 1):
        total += crc[k, :, cols : 2 * cols] * jnp.exp(crc[k, :, 0:cols] - high)
    crc[0, :, 0:cols] = high + jnp.log(total)

    def turn(i):
        if Z != 4:
            return jnp.int32(i)
        first_z, second_z, third_z, fourth_z = (row[i] for row in TURNS)
        low = lax.select(z == 0, jnp.int32(first_z), jnp.int32(second_z))
        high = lax.select(z == 2, jnp.int32(third_z), jnp.int32(fourth_z))
        return lax.select(z < 2, low, high)

    def share(i, k):
        return remote(W.at[k], Ws.at[k], out_s, w_r.at[min(i, 1)], sibling)

    for i in range(Z):
        k = turn(i)
        W[k] = (A[k] + jnp.exp(S[:, span(k, n)] - crc[0, :, span(k, n)])).astype(BF16)
        share(i, k).start()

    def pack(value):
        top = jnp.maximum(jnp.max(jnp.abs(value), axis=0, keepdims=True), 1e-30)
        return jnp.round(value * (32766.0 / top)).astype(jnp.int32).astype(I16), top * (1.0 / 32766.0)

    def unpack(at, step, k):
        return at[k].astype(jnp.int32).astype(F32) * step[k]

    def query_terms(h):
        def term(k):
            return dot(W[k], PB[h, span(k, n), :], 1, 0)

        if Z <= 4:
            return dot(jnp.concatenate([W[k] for k in range(Z)], axis=1), PB[h], 1, 0)
        return lax.fori_loop(0, Z, lambda k, t: t + term(k), jnp.zeros((rows, w), F32))

    def gq_send(j, value, slot, data, step, device):
        gqt[j], gqk[j] = pack(value)
        remote(gqt.at[j], gqr.at[slot], out_s, data, device).start()
        remote(gqk.at[j], gqkr.at[slot], out_s, step, device).start()

    for h in (0, 1):
        gqp[h] = query_terms(h)
    beside, across = dev(z, 1 - y, c, x), dev(z, y, c, 1 - x)
    corner = dev(z, 1 - y, c, lax.select(c == 1, x, 1 - x))

    def gq_across(more):
        gq_send(2, gqp[1 - x, span(y, n), :] + more, 2, gq_r.at[1], gq_r.at[1], across)

    gq_send(0, gqp[1 - x, span(1 - y, n), :], 0, d_r, d_r, corner)

    @pl.when(c == 0)
    def _():
        gq_across(0.0)

    gq_send(1, gqp[x, span(1 - y, n), :], 1, gq_r.at[0], gq_r.at[0], beside)

    for i in range(Z):
        k = turn(i)
        mine = dot(W[k], Q[1 - c], 0, 0)
        if i < 2:
            settle(w_r.at[i], i * (Z - 1) * 2 * rows * n + (1 - i) * 2 * rows * (n + w))
        packed, step = pack(mine + dot(Ws[k], Qs[...], 0, 0))
        away = jnp.logical_or(z != k, crossed)

        @pl.when(away)
        def _():
            gpt[k], gpk[k] = packed, step
            remote(gpt.at[k], gpr.at[z], out_s, gp_r, target(k)).start()
            remote(gpk.at[k], gpkr.at[z], out_s, gp_r, target(k)).start()

        @pl.when(jnp.logical_not(away))
        def _():
            gpr[k], gpkr[k] = packed, step

    settle(d_r, packed_bytes)

    @pl.when(c == 1)
    def _():
        gq_across(unpack(gqr, gqkr, 0))

    for j in (0, 1):
        settle(gq_r.at[j], packed_bytes)
    total = gqp[x, span(y, n), :] + unpack(gqr, gqkr, 1) + unpack(gqr, gqkr, 2)
    gq_ref[...] = total + unpack(gqr, gqkr, 0) * (1 - c).astype(F32)

    def per_count(body):
        @pl.when(own)
        def _():
            body(Z - 1)

        @pl.when(crossed)
        def _():
            body(Z)

    per_count(lambda count: settle(gp_r, count * packed_bytes))
    gp_ref[...] = sum(unpack(gpr, gpkr, k) for k in range(Z))

    per_count(lambda count: settle(out_s, sent_bytes(n, w, Z, count == Z)))


def local(queries, passages, positives):
    n, w = queries.shape
    batch_count = lax.axis_size("batch")
    Z = batch_count // 4
    scale = 1.0 / math.sqrt(w * lax.axis_size("rep"))
    rows, cols = 2 * n, Z * n
    vmem = pl.BlockSpec(memory_space=pltpu.VMEM)
    dma = pltpu.SemaphoreType.DMA
    regular = pltpu.SemaphoreType.REGULAR
    hbm = pl.BlockSpec(memory_space=pltpu.HBM)
    operands = (queries, passages, positives.reshape(batch_count, n))
    grad_queries, grad_passages = pl.pallas_call(
        functools.partial(kernel, Z, scale),
        out_shape=(
            jax.ShapeDtypeStruct((n, w), F32),
            jax.ShapeDtypeStruct((n, w), F32),
        ),
        in_specs=[hbm] * 3,
        out_specs=(vmem, vmem),
        scratch_shapes=[
            pltpu.VMEM((2, rows, w), BF16),
            pltpu.VMEM((rows, w), BF16),
            pltpu.VMEM((2, cols, w), BF16),
            pltpu.VMEM((rows, cols), F32),
            pltpu.VMEM((Z, rows, n), F32),
            pltpu.VMEM((Z, rows, n), BF16),
            pltpu.VMEM((Z, rows, n), BF16),
            pltpu.VMEM((1, 2 * rows), F32),
            pltpu.VMEM((3, 1, 2 * rows), F32),
            pltpu.VMEM((1, 2 * cols), F32),
            pltpu.VMEM((2 * Z - 1, 1, 2 * cols), F32),
            pltpu.VMEM((n, w), BF16),
            pltpu.VMEM((batch_count, n), jnp.int32),
            pltpu.VMEM((1, sent_bytes(n, w, Z) // 4), F32),
            pltpu.VMEM((2, rows, w), F32),
            pltpu.VMEM((3, n, w), I16),
            pltpu.VMEM((3, n, w), I16),
            pltpu.VMEM((3, 1, w), F32),
            pltpu.VMEM((3, 1, w), F32),
            pltpu.VMEM((Z, n, w), I16),
            pltpu.VMEM((Z, n, w), I16),
            pltpu.VMEM((Z, 1, w), F32),
            pltpu.VMEM((Z, 1, w), F32),
            regular((2,)),
            regular((Z,)),
            regular,
            dma,
            dma,
            dma((2,)),
            dma((Z,)),
            dma((Z // 2,)),
            dma,
            dma,
            dma((2,)),
            dma((2,)),
            dma,
            dma,
        ],
        compiler_params=pltpu.CompilerParams(collective_id=0, has_side_effects=True, vmem_limit_bytes=6 * 2**20 + 40 * rows * cols),
    )(*(pltpu.with_memory_space_constraint(a, pltpu.HBM) for a in operands))
    return grad_queries * scale, grad_passages * scale


def solution(mesh):
    in_specs = (P("batch", "rep"), P("batch", "rep"), P())
    out_specs = (P("batch", "rep"), P("batch", "rep"))
    return jax.shard_map(local, mesh=mesh, in_specs=in_specs, out_specs=out_specs, check_vma=False)
```

```python
import functools
import math

import jax
import jax.numpy as jnp
from jax import lax
from jax.experimental import pallas as pl
from jax.experimental.pallas import tpu as pltpu
from jax.sharding import PartitionSpec as P

MESH = pl.DeviceIdType.MESH
F32 = jnp.float32
BF16 = jnp.bfloat16
I16 = jnp.int16
TURNS = ((0, 1, 3, 2), (0, 3, 2, 1), (0, 3, 1, 2), (2, 0, 1, 3))


def dot(a, b, da, db):
    return lax.dot_general(a, b, (((da,), (db,)), ((), ())), preferred_element_type=F32)


def sent_bytes(n, w, Z, crossed=True):
    block, step = 2 * n * w, 4 * w
    blocks = 3 + (Z - 1 + crossed) + Z + 2 + 3 + (Z - 1 + crossed)
    steps = 3 + (Z - 1 + crossed)
    weights = Z * 2 * n * n * 2
    stats = (2 * Z - 1) * 2 * Z * n * 4 + 3 * 4 * n * 4
    return blocks * block + steps * step + weights + stats


def as_column(row, lanes):
    return jnp.broadcast_to(row, (lanes, row.shape[1])).T


def kernel(
    Z,
    scale,
    q_ref,
    p_ref,
    pos_hbm,
    gq_ref,
    gp_ref,
    Q,
    Qs,
    PB,
    S,
    A,
    W,
    Ws,
    rst,
    rrc,
    cst,
    crc,
    PM,
    pos_ref,
    span_ref,
    gqp,
    gqt,
    gqr,
    gqk,
    gqkr,
    gpt,
    gpr,
    gpk,
    gpkr,
    near,
    line,
    rest,
    in_s,
    out_s,
    q_r,
    p_r,
    f_r,
    r_r,
    c_r,
    w_r,
    gq_r,
    gp_r,
    d_r,
):
    n, w = q_ref.shape
    b = lax.axis_index("batch")
    x = lax.axis_index("rep")
    z, y, c = b // 4, (b // 2) % 2, b % 2
    rows, cols = 2 * n, Z * n

    def dev(zz, yy, cc, xx):
        return (zz * 4 + yy * 2 + cc, xx)

    def plane(j):
        xx = 1 - x if j & 1 else x
        yy = 1 - y if j & 2 else y
        return xx, yy

    def remote(src, dst, s, r, device):
        return pltpu.make_async_remote_copy(
            src_ref=src, dst_ref=dst, send_sem=s, recv_sem=r, device_id=device, device_id_type=MESH
        )

    def span(k, size):
        return pl.ds(k * size if isinstance(k, int) else pl.multiple_of(k * size, size), size)

    def settle(sem, size):
        ref = span_ref.at[:, pl.ds(0, size // 4)]
        pltpu.make_async_copy(ref, ref, sem).wait()

    packed_bytes = 2 * n * w + 4 * w

    def up(dz):
        return (z + dz) % Z

    own = c == 1 - x
    crossed = jnp.logical_not(own)
    sibling = dev(z, y, 1 - c, x)

    def target(zz):
        return dev(zz, y, 1 - x, 1 - c)

    barrier = pltpu.get_barrier_semaphore()

    q_own = Q.at[x, span(y, n)]
    p_in = pltpu.make_async_copy(p_ref, PM, in_s)
    q_in = pltpu.make_async_copy(q_ref, q_own, in_s)
    pos_in = pltpu.make_async_copy(pos_hbm, pos_ref, in_s)
    q_in.start()
    p_in.start()
    pos_in.start()

    def greet(sem, device):
        pl.semaphore_signal(sem, inc=1, device_id=device, device_id_type=MESH)

    place = 2 * y + x
    pairs = []
    for j in (1, 2):
        xx, yy = plane(j)
        pairs.append((2 * yy + xx < place, dev(z, yy, c, xx), near.at[j - 1]))
    pairs.append((c == 0, sibling, rest))
    for dz in range(1, Z):
        zz = up(dz)
        pairs.append((zz < z, target(zz), line.at[z]))
        for cc in (0, 1):
            pairs.append((zz < z, dev(zz, y, cc, x), rest))
    first = jnp.logical_and(crossed, x == 1)
    last = jnp.logical_and(crossed, x == 0)
    for earlier, device, _ in pairs:

        @pl.when(jnp.logical_not(earlier))
        def _():
            greet(barrier, device)

    @pl.when(last)
    def _():
        greet(barrier, target(z))

    greetings = x + y + 3 * z + (1 - c) + first.astype(jnp.int32)

    @pl.when(greetings > 0)
    def _():
        pl.semaphore_wait(barrier, greetings)

    for earlier, device, sem in pairs:

        @pl.when(earlier)
        def _():
            greet(sem, device)

    @pl.when(first)
    def _():
        greet(line.at[z], target(z))

    settle(in_s, 4 * n * w + 4 * pos_ref.shape[0] * n)
    p_block = PB.at[x, span(z, n)]

    def p_copy(zz):
        return remote(PM, p_block, out_s, p_r.at[z], target(zz))

    @pl.when(first)
    def _():
        p_copy(z).start()

    for k in range(Z - 1):

        @pl.when(k < z)
        def _():
            p_copy(k).start()

    @pl.when(own)
    def _():
        PB[x, span(z, n), :] = PM[...]

    @pl.when(last)
    def _():
        pl.semaphore_wait(line.at[z], 1)
        p_copy(z).start()

    q_copies = []
    for j in (1, 2):
        xx, yy = plane(j)
        q_copies.append(remote(q_own, q_own, out_s, q_r.at[j - 1], dev(z, yy, c, xx)))

        @pl.when(2 * yy + xx > place)
        def _():
            pl.semaphore_wait(near.at[j - 1], 1)

        q_copies[-1].start()

    def send_later(zz):
        pl.semaphore_wait(line.at[zz], 1)
        p_copy(zz).start()

    nearest_last = jnp.logical_and(z > 0, jnp.logical_and(c == 0, x == 1))

    @pl.when(jnp.logical_and(z < Z - 1, jnp.logical_not(nearest_last)))
    def _():
        send_later(z + 1)

    for k in range(2, Z):

        @pl.when(k > z + 1)
        def _():
            send_later(k)

    @pl.when(jnp.logical_and(z < Z - 1, nearest_last))
    def _():
        send_later(z + 1)

    answers = 2 * (Z - 1 - z) + c

    @pl.when(answers > 0)
    def _():
        pl.semaphore_wait(rest, answers)

    q_copies[0].wait_recv()
    q_far = Q.at[1 - x, span(y, n)]
    remote(q_far, q_far, out_s, q_r.at[1], dev(z, 1 - y, c, x)).start()

    def part(zz):
        return PB.at[1 - c, span(zz, n)]

    def forward(k):
        zz = nth(k)
        return remote(part(zz), part(zz), out_s, f_r.at[k // 2], sibling)

    def nth(k):
        return lax.select(k < Z - z, z + k, jnp.int32(Z - 1 - k))

    def scores(*ks):
        pltpu.make_async_copy(Q.at[0], Q.at[0], f_r.at[ks[0] // 2]).wait()
        parts = []
        for k in ks:
            zz = nth(k)
            at = span(zz, n)
            s = (dot(Q[0], PB[0, at, :], 1, 1) + dot(Q[1], PB[1, at, :], 1, 1)) * scale
            S[:, at] = s
            top = jnp.max(s, axis=0, keepdims=True)
            cst[:, at] = top
            cst[:, span(zz + Z, n)] = jnp.sum(jnp.exp(s - top), axis=0, keepdims=True)
            parts.append(s)
        return parts

    def row_part(parts, running):
        high = jnp.max(functools.reduce(jnp.maximum, parts), axis=1, keepdims=True)
        if running is not None:
            high = jnp.maximum(high, running[0])
        total = jnp.sum(sum(jnp.exp(s - high) for s in parts), axis=1, keepdims=True)
        if running is not None:
            total += running[1] * jnp.exp(running[0] - high)
        return high, total

    half = remote(Q.at[c], Qs, out_s, w_r.at[0], sibling)

    @pl.when(own)
    def _():
        forward(0).start()

    def arrive(k):
        zz = nth(k)

        @pl.when(jnp.logical_or(zz != z, crossed))
        def _():
            pltpu.make_async_copy(PM, part(zz), p_r.at[zz]).wait()
            forward(k).start()

    for k in range(Z):
        arrive(k)
    pltpu.make_async_copy(Q.at[0], Q.at[0], q_r.at[1]).wait()
    half.start()
    running = None
    for k in range(0, Z - 2, 2):
        running = row_part(scores(k, k + 1), running)
    parts = scores(Z - 2, Z - 1)

    col_copies = []
    for dz in range(Z):
        for dc in (0, 1):
            if dz or dc:
                k = dz * 2 + dc
                col_copies.append(
                    remote(cst, crc.at[k - 1], out_s, c_r, dev(up(dz), y, 1 - c if dc else c, x))
                )
                col_copies[-1].start()

    running = row_part(parts, running)

    def as_row(column):
        return jnp.broadcast_to(column, (rows, 128)).T[0:1, :]

    rst[:, 0:rows] = as_row(running[0])
    rst[:, rows : 2 * rows] = as_row(running[1])
    row_copies = []
    for j in (1, 2, 3):
        xx, yy = plane(j)
        row_copies.append(remote(rst, rrc.at[j - 1], out_s, r_r, dev(z, yy, c, xx)))
        row_copies[-1].start()

    places = jnp.concatenate(
        [
            as_column(pos_ref[pl.ds(z * 4 + yy * 2 + c, 1), :].astype(F32), 128)
            for yy in (0, 1)
        ],
        axis=0,
    )

    pltpu.make_async_copy(rrc, rrc, r_r).wait()
    high = rst[:, 0:rows]
    for j in range(3):
        high = jnp.maximum(high, rrc[j, :, 0:rows])
    total = rst[:, rows : 2 * rows] * jnp.exp(rst[:, 0:rows] - high)
    for j in range(3):
        total += rrc[j, :, rows : 2 * rows] * jnp.exp(rrc[j, :, 0:rows] - high)
    row_norm = as_column(high + jnp.log(total), 128)

    lane = lax.broadcasted_iota(jnp.int32, (rows, n), 1).astype(F32)
    for k in range(Z):
        base = lax.convert_element_type((k * 4 + y * 2 + 1 - x) * n, F32)
        hit = jnp.where(places - lane == base, 2.0, 0.0)
        A[k] = jnp.exp(S[:, span(k, n)] - row_norm) - hit

    pltpu.make_async_copy(crc, crc, c_r).wait()
    high = cst[:, 0:cols]
    for k in range(2 * Z - 1):
        high = jnp.maximum(high, crc[k, :, 0:cols])
    total = cst[:, cols : 2 * cols] * jnp.exp(cst[:, 0:cols] - high)
    for k in range(2 * Z - 1):
        total += crc[k, :, cols : 2 * cols] * jnp.exp(crc[k, :, 0:cols] - high)
    crc[0, :, 0:cols] = high + jnp.log(total)

    def turn(i):
        if Z != 4:
            return jnp.int32(i)
        first_z, second_z, third_z, fourth_z = (row[i] for row in TURNS)
        low = lax.select(z == 0, jnp.int32(first_z), jnp.int32(second_z))
        high = lax.select(z == 2, jnp.int32(third_z), jnp.int32(fourth_z))
        return lax.select(z < 2, low, high)

    def share(i, k):
        return remote(W.at[k], Ws.at[k], out_s, w_r.at[min(i, 1)], sibling)

    for i in range(Z):
        k = turn(i)
        W[k] = (A[k] + jnp.exp(S[:, span(k, n)] - crc[0, :, span(k, n)])).astype(BF16)
        share(i, k).start()

    def pack(value):
        top = jnp.maximum(jnp.max(jnp.abs(value), axis=0, keepdims=True), 1e-30)
        return jnp.round(value * (32766.0 / top)).astype(jnp.int32).astype(I16), top * (1.0 / 32766.0)

    def unpack(at, step, k):
        return at[k].astype(jnp.int32).astype(F32) * step[k]

    def query_terms(h):
        def term(k):
            return dot(W[k], PB[h, span(k, n), :], 1, 0)

        if Z <= 4:
            return dot(jnp.concatenate([W[k] for k in range(Z)], axis=1), PB[h], 1, 0)
        return lax.fori_loop(0, Z, lambda k, t: t + term(k), jnp.zeros((rows, w), F32))

    def gq_send(j, value, slot, data, step, device):
        gqt[j], gqk[j] = pack(value)
        remote(gqt.at[j], gqr.at[slot], out_s, data, device).start()
        remote(gqk.at[j], gqkr.at[slot], out_s, step, device).start()

    for h in (0, 1):
        gqp[h] = query_terms(h)
    beside, across = dev(z, 1 - y, c, x), dev(z, y, c, 1 - x)
    corner = dev(z, 1 - y, c, lax.select(c == 1, x, 1 - x))

    def gq_across(more):
        gq_send(2, gqp[1 - x, span(y, n), :] + more, 2, gq_r.at[1], gq_r.at[1], across)

    def gq_beside():
        gq_send(1, gqp[x, span(1 - y, n), :], 1, gq_r.at[0], gq_r.at[0], beside)

    across_first = jnp.logical_and(c == 0, jnp.logical_and(y == 0, x == 1))
    beside_first = jnp.logical_and(y == 1, x == 0)

    @pl.when(across_first)
    def _():
        gq_across(0.0)

    @pl.when(beside_first)
    def _():
        gq_beside()

    gq_send(0, gqp[1 - x, span(1 - y, n), :], 0, d_r, d_r, corner)

    @pl.when(jnp.logical_and(c == 0, jnp.logical_not(across_first)))
    def _():
        gq_across(0.0)

    @pl.when(jnp.logical_not(beside_first))
    def _():
        gq_beside()

    for i in range(Z):
        k = turn(i)
        mine = dot(W[k], Q[1 - c], 0, 0)
        if i < 2:
            settle(w_r.at[i], i * (Z - 1) * 2 * rows * n + (1 - i) * 2 * rows * (n + w))
        packed, step = pack(mine + dot(Ws[k], Qs[...], 0, 0))
        away = jnp.logical_or(z != k, crossed)

        @pl.when(away)
        def _():
            gpt[k], gpk[k] = packed, step
            remote(gpt.at[k], gpr.at[z], out_s, gp_r, target(k)).start()
            remote(gpk.at[k], gpkr.at[z], out_s, gp_r, target(k)).start()

        @pl.when(jnp.logical_not(away))
        def _():
            gpr[k], gpkr[k] = packed, step

    settle(d_r, packed_bytes)

    @pl.when(c == 1)
    def _():
        gq_across(unpack(gqr, gqkr, 0))

    for j in (0, 1):
        settle(gq_r.at[j], packed_bytes)
    total = gqp[x, span(y, n), :] + unpack(gqr, gqkr, 1) + unpack(gqr, gqkr, 2)
    gq_ref[...] = total + unpack(gqr, gqkr, 0) * (1 - c).astype(F32)

    def per_count(body):
        @pl.when(own)
        def _():
            body(Z - 1)

        @pl.when(crossed)
        def _():
            body(Z)

    per_count(lambda count: settle(gp_r, count * packed_bytes))
    gp_ref[...] = sum(unpack(gpr, gpkr, k) for k in range(Z))

    per_count(lambda count: settle(out_s, sent_bytes(n, w, Z, count == Z)))


def local(queries, passages, positives):
    n, w = queries.shape
    batch_count = lax.axis_size("batch")
    Z = batch_count // 4
    scale = 1.0 / math.sqrt(w * lax.axis_size("rep"))
    rows, cols = 2 * n, Z * n
    vmem = pl.BlockSpec(memory_space=pltpu.VMEM)
    dma = pltpu.SemaphoreType.DMA
    regular = pltpu.SemaphoreType.REGULAR
    hbm = pl.BlockSpec(memory_space=pltpu.HBM)
    operands = (queries, passages, positives.reshape(batch_count, n))
    grad_queries, grad_passages = pl.pallas_call(
        functools.partial(kernel, Z, scale),
        out_shape=(
            jax.ShapeDtypeStruct((n, w), F32),
            jax.ShapeDtypeStruct((n, w), F32),
        ),
        in_specs=[hbm] * 3,
        out_specs=(vmem, vmem),
        scratch_shapes=[
            pltpu.VMEM((2, rows, w), BF16),
            pltpu.VMEM((rows, w), BF16),
            pltpu.VMEM((2, cols, w), BF16),
            pltpu.VMEM((rows, cols), F32),
            pltpu.VMEM((Z, rows, n), F32),
            pltpu.VMEM((Z, rows, n), BF16),
            pltpu.VMEM((Z, rows, n), BF16),
            pltpu.VMEM((1, 2 * rows), F32),
            pltpu.VMEM((3, 1, 2 * rows), F32),
            pltpu.VMEM((1, 2 * cols), F32),
            pltpu.VMEM((2 * Z - 1, 1, 2 * cols), F32),
            pltpu.VMEM((n, w), BF16),
            pltpu.VMEM((batch_count, n), jnp.int32),
            pltpu.VMEM((1, sent_bytes(n, w, Z) // 4), F32),
            pltpu.VMEM((2, rows, w), F32),
            pltpu.VMEM((3, n, w), I16),
            pltpu.VMEM((3, n, w), I16),
            pltpu.VMEM((3, 1, w), F32),
            pltpu.VMEM((3, 1, w), F32),
            pltpu.VMEM((Z, n, w), I16),
            pltpu.VMEM((Z, n, w), I16),
            pltpu.VMEM((Z, 1, w), F32),
            pltpu.VMEM((Z, 1, w), F32),
            regular((2,)),
            regular((Z,)),
            regular,
            dma,
            dma,
            dma((2,)),
            dma((Z,)),
            dma((Z // 2,)),
            dma,
            dma,
            dma((2,)),
            dma((2,)),
            dma,
            dma,
        ],
        compiler_params=pltpu.CompilerParams(collective_id=0, has_side_effects=True, vmem_limit_bytes=6 * 2**20 + 40 * rows * cols),
    )(*(pltpu.with_memory_space_constraint(a, pltpu.HBM) for a in operands))
    return grad_queries * scale, grad_passages * scale


def solution(mesh):
    in_specs = (P("batch", "rep"), P("batch", "rep"), P())
    out_specs = (P("batch", "rep"), P("batch", "rep"))
    return jax.shard_map(local, mesh=mesh, in_specs=in_specs, out_specs=out_specs, check_vma=False)
```

```python
import functools
import math

import jax
import jax.numpy as jnp
from jax import lax
from jax.experimental import pallas as pl
from jax.experimental.pallas import tpu as pltpu
from jax.sharding import PartitionSpec as P

MESH = pl.DeviceIdType.MESH
F32 = jnp.float32
BF16 = jnp.bfloat16
I16 = jnp.int16
TURNS = ((0, 1, 3, 2), (0, 3, 2, 1), (0, 3, 1, 2), (2, 0, 1, 3))


def dot(a, b, da, db):
    return lax.dot_general(a, b, (((da,), (db,)), ((), ())), preferred_element_type=F32)


def sent_bytes(n, w, Z, crossed=True):
    block, step = 2 * n * w, 4 * w
    blocks = 3 + (Z - 1 + crossed) + Z + 2 + 3 + (Z - 1 + crossed)
    steps = 3 + (Z - 1 + crossed)
    weights = Z * 2 * n * n * 2
    stats = (2 * Z - 1) * 2 * Z * n * 4 + 3 * 4 * n * 4
    return blocks * block + steps * step + weights + stats


def as_column(row, lanes):
    return jnp.broadcast_to(row, (lanes, row.shape[1])).T


def kernel(
    Z,
    scale,
    q_ref,
    p_ref,
    pos_hbm,
    gq_ref,
    gp_ref,
    Q,
    Qs,
    PB,
    S,
    A,
    W,
    Ws,
    rst,
    rrc,
    cst,
    crc,
    PM,
    pos_ref,
    span_ref,
    gqp,
    gqt,
    gqr,
    gqk,
    gqkr,
    gpt,
    gpr,
    gpk,
    gpkr,
    near,
    line,
    rest,
    in_s,
    out_s,
    q_r,
    p_r,
    f_r,
    r_r,
    c_r,
    w_r,
    gq_r,
    gp_r,
    d_r,
):
    n, w = q_ref.shape
    b = lax.axis_index("batch")
    x = lax.axis_index("rep")
    z, y, c = b // 4, (b // 2) % 2, b % 2
    rows, cols = 2 * n, Z * n

    def dev(zz, yy, cc, xx):
        return (zz * 4 + yy * 2 + cc, xx)

    def plane(j):
        xx = 1 - x if j & 1 else x
        yy = 1 - y if j & 2 else y
        return xx, yy

    def remote(src, dst, s, r, device):
        return pltpu.make_async_remote_copy(
            src_ref=src, dst_ref=dst, send_sem=s, recv_sem=r, device_id=device, device_id_type=MESH
        )

    def span(k, size):
        return pl.ds(k * size if isinstance(k, int) else pl.multiple_of(k * size, size), size)

    def settle(sem, size):
        ref = span_ref.at[:, pl.ds(0, size // 4)]
        pltpu.make_async_copy(ref, ref, sem).wait()

    packed_bytes = 2 * n * w + 4 * w

    def up(dz):
        return (z + dz) % Z

    own = c == 1 - x
    crossed = jnp.logical_not(own)
    sibling = dev(z, y, 1 - c, x)

    def target(zz):
        return dev(zz, y, 1 - x, 1 - c)

    barrier = pltpu.get_barrier_semaphore()

    q_own = Q.at[x, span(y, n)]
    p_in = pltpu.make_async_copy(p_ref, PM, in_s)
    q_in = pltpu.make_async_copy(q_ref, q_own, in_s)
    pos_in = pltpu.make_async_copy(pos_hbm, pos_ref, in_s)
    q_in.start()
    p_in.start()
    pos_in.start()

    def greet(sem, device):
        pl.semaphore_signal(sem, inc=1, device_id=device, device_id_type=MESH)

    place = 2 * y + x
    pairs = []
    for j in (1, 2):
        xx, yy = plane(j)
        pairs.append((2 * yy + xx < place, dev(z, yy, c, xx), near.at[j - 1]))
    pairs.append((c == 0, sibling, rest))
    for dz in range(1, Z):
        zz = up(dz)
        pairs.append((zz < z, target(zz), line.at[z]))
        for cc in (0, 1):
            pairs.append((zz < z, dev(zz, y, cc, x), rest))
    first = jnp.logical_and(crossed, x == 1)
    last = jnp.logical_and(crossed, x == 0)
    for earlier, device, _ in pairs:

        @pl.when(jnp.logical_not(earlier))
        def _():
            greet(barrier, device)

    @pl.when(last)
    def _():
        greet(barrier, target(z))

    greetings = x + y + 3 * z + (1 - c) + first.astype(jnp.int32)

    @pl.when(greetings > 0)
    def _():
        pl.semaphore_wait(barrier, greetings)

    for earlier, device, sem in pairs:

        @pl.when(earlier)
        def _():
            greet(sem, device)

    @pl.when(first)
    def _():
        greet(line.at[z], target(z))

    settle(in_s, 4 * n * w + 4 * pos_ref.shape[0] * n)
    p_block = PB.at[x, span(z, n)]

    def p_copy(zz):
        return remote(PM, p_block, out_s, p_r.at[z], target(zz))

    @pl.when(first)
    def _():
        p_copy(z).start()

    for k in range(Z - 1):

        @pl.when(k < z)
        def _():
            p_copy(k).start()

    @pl.when(own)
    def _():
        PB[x, span(z, n), :] = PM[...]

    @pl.when(last)
    def _():
        pl.semaphore_wait(line.at[z], 1)
        p_copy(z).start()

    q_copies = []
    for j in (1, 2):
        xx, yy = plane(j)
        q_copies.append(remote(q_own, q_own, out_s, q_r.at[j - 1], dev(z, yy, c, xx)))

        @pl.when(2 * yy + xx > place)
        def _():
            pl.semaphore_wait(near.at[j - 1], 1)

        q_copies[-1].start()

    def send_later(zz):
        pl.semaphore_wait(line.at[zz], 1)
        p_copy(zz).start()

    nearest_last = jnp.logical_and(z > 0, jnp.logical_and(c == 0, x == 1))

    @pl.when(jnp.logical_and(z < Z - 1, jnp.logical_not(nearest_last)))
    def _():
        send_later(z + 1)

    for k in range(2, Z):

        @pl.when(k > z + 1)
        def _():
            send_later(k)

    @pl.when(jnp.logical_and(z < Z - 1, nearest_last))
    def _():
        send_later(z + 1)

    answers = 2 * (Z - 1 - z) + c

    @pl.when(answers > 0)
    def _():
        pl.semaphore_wait(rest, answers)

    q_copies[0].wait_recv()
    q_far = Q.at[1 - x, span(y, n)]
    remote(q_far, q_far, out_s, q_r.at[1], dev(z, 1 - y, c, x)).start()

    def part(zz):
        return PB.at[1 - c, span(zz, n)]

    def forward(k):
        zz = nth(k)
        return remote(part(zz), part(zz), out_s, f_r.at[k // 2], sibling)

    def nth(k):
        return lax.select(k < Z - z, z + k, jnp.int32(Z - 1 - k))

    def scores(*ks):
        pltpu.make_async_copy(Q.at[0], Q.at[0], f_r.at[ks[0] // 2]).wait()
        parts = []
        for k in ks:
            zz = nth(k)
            at = span(zz, n)
            s = (dot(Q[0], PB[0, at, :], 1, 1) + dot(Q[1], PB[1, at, :], 1, 1)) * scale
            S[:, at] = s
            top = jnp.max(s, axis=0, keepdims=True)
            cst[:, at] = top
            cst[:, span(zz + Z, n)] = jnp.sum(jnp.exp(s - top), axis=0, keepdims=True)
            parts.append(s)
        return parts

    def row_part(parts, running):
        high = jnp.max(functools.reduce(jnp.maximum, parts), axis=1, keepdims=True)
        if running is not None:
            high = jnp.maximum(high, running[0])
        total = jnp.sum(sum(jnp.exp(s - high) for s in parts), axis=1, keepdims=True)
        if running is not None:
            total += running[1] * jnp.exp(running[0] - high)
        return high, total

    half = remote(Q.at[c], Qs, out_s, w_r.at[0], sibling)

    @pl.when(own)
    def _():
        forward(0).start()

    def arrive(k):
        zz = nth(k)

        @pl.when(jnp.logical_or(zz != z, crossed))
        def _():
            pltpu.make_async_copy(PM, part(zz), p_r.at[zz]).wait()
            forward(k).start()

    for k in range(Z):
        arrive(k)
    pltpu.make_async_copy(Q.at[0], Q.at[0], q_r.at[1]).wait()
    half.start()
    running = None
    for k in range(0, Z - 2, 2):
        running = row_part(scores(k, k + 1), running)
    parts = scores(Z - 2, Z - 1)

    col_copies = []
    for dz in range(Z):
        for dc in (0, 1):
            if dz or dc:
                k = dz * 2 + dc
                col_copies.append(
                    remote(cst, crc.at[k - 1], out_s, c_r, dev(up(dz), y, 1 - c if dc else c, x))
                )
                col_copies[-1].start()

    running = row_part(parts, running)

    def as_row(column):
        return jnp.broadcast_to(column, (rows, 128)).T[0:1, :]

    rst[:, 0:rows] = as_row(running[0])
    rst[:, rows : 2 * rows] = as_row(running[1])
    row_copies = []
    for j in (1, 2, 3):
        xx, yy = plane(j)
        row_copies.append(remote(rst, rrc.at[j - 1], out_s, r_r, dev(z, yy, c, xx)))
        row_copies[-1].start()

    places = jnp.concatenate(
        [
            as_column(pos_ref[pl.ds(z * 4 + yy * 2 + c, 1), :].astype(F32), 128)
            for yy in (0, 1)
        ],
        axis=0,
    )

    pltpu.make_async_copy(rrc, rrc, r_r).wait()
    high = rst[:, 0:rows]
    for j in range(3):
        high = jnp.maximum(high, rrc[j, :, 0:rows])
    total = rst[:, rows : 2 * rows] * jnp.exp(rst[:, 0:rows] - high)
    for j in range(3):
        total += rrc[j, :, rows : 2 * rows] * jnp.exp(rrc[j, :, 0:rows] - high)
    row_norm = as_column(high + jnp.log(total), 128)

    lane = lax.broadcasted_iota(jnp.int32, (rows, n), 1).astype(F32)
    for k in range(Z):
        base = lax.convert_element_type((k * 4 + y * 2 + 1 - x) * n, F32)
        hit = jnp.where(places - lane == base, 2.0, 0.0)
        A[k] = jnp.exp(S[:, span(k, n)] - row_norm) - hit

    pltpu.make_async_copy(crc, crc, c_r).wait()
    high = cst[:, 0:cols]
    for k in range(2 * Z - 1):
        high = jnp.maximum(high, crc[k, :, 0:cols])
    total = cst[:, cols : 2 * cols] * jnp.exp(cst[:, 0:cols] - high)
    for k in range(2 * Z - 1):
        total += crc[k, :, cols : 2 * cols] * jnp.exp(crc[k, :, 0:cols] - high)
    crc[0, :, 0:cols] = high + jnp.log(total)

    def turn(i):
        if Z != 4:
            return jnp.int32(i)
        first_z, second_z, third_z, fourth_z = (row[i] for row in TURNS)
        low = lax.select(z == 0, jnp.int32(first_z), jnp.int32(second_z))
        high = lax.select(z == 2, jnp.int32(third_z), jnp.int32(fourth_z))
        return lax.select(z < 2, low, high)

    def share(i, k):
        return remote(W.at[k], Ws.at[k], out_s, w_r.at[min(i, 1)], sibling)

    for i in range(Z):
        k = turn(i)
        W[k] = (A[k] + jnp.exp(S[:, span(k, n)] - crc[0, :, span(k, n)])).astype(BF16)
        share(i, k).start()

    def pack(value):
        top = jnp.maximum(jnp.max(jnp.abs(value), axis=0, keepdims=True), 1e-30)
        return jnp.round(value * (32766.0 / top)).astype(jnp.int32).astype(I16), top * (1.0 / 32766.0)

    def unpack(at, step, k):
        return at[k].astype(jnp.int32).astype(F32) * step[k]

    def query_terms(h):
        def term(k):
            return dot(W[k], PB[h, span(k, n), :], 1, 0)

        if Z <= 4:
            return dot(jnp.concatenate([W[k] for k in range(Z)], axis=1), PB[h], 1, 0)
        return lax.fori_loop(0, Z, lambda k, t: t + term(k), jnp.zeros((rows, w), F32))

    def gq_send(j, value, slot, data, step, device):
        gqt[j], gqk[j] = pack(value)
        remote(gqt.at[j], gqr.at[slot], out_s, data, device).start()
        remote(gqk.at[j], gqkr.at[slot], out_s, step, device).start()

    gqp[1 - x] = query_terms(1 - x)
    beside, across = dev(z, 1 - y, c, x), dev(z, y, c, 1 - x)
    corner = dev(z, 1 - y, c, lax.select(c == 1, x, 1 - x))

    def gq_across(more):
        gq_send(2, gqp[1 - x, span(y, n), :] + more, 2, gq_r.at[1], gq_r.at[1], across)

    def gq_beside():
        gq_send(1, gqp[x, span(1 - y, n), :], 1, gq_r.at[0], gq_r.at[0], beside)

    across_first = jnp.logical_and(c == 0, jnp.logical_and(y == 0, x == 1))
    beside_first = jnp.logical_and(y == 1, x == 0)

    @pl.when(across_first)
    def _():
        gq_across(0.0)

    gqp[x] = query_terms(x)

    @pl.when(beside_first)
    def _():
        gq_beside()

    gq_send(0, gqp[1 - x, span(1 - y, n), :], 0, d_r, d_r, corner)

    @pl.when(jnp.logical_and(c == 0, jnp.logical_not(across_first)))
    def _():
        gq_across(0.0)

    @pl.when(jnp.logical_not(beside_first))
    def _():
        gq_beside()

    for i in range(Z):
        k = turn(i)
        mine = dot(W[k], Q[1 - c], 0, 0)
        if i < 2:
            settle(w_r.at[i], i * (Z - 1) * 2 * rows * n + (1 - i) * 2 * rows * (n + w))
        packed, step = pack(mine + dot(Ws[k], Qs[...], 0, 0))
        away = jnp.logical_or(z != k, crossed)

        @pl.when(away)
        def _():
            gpt[k], gpk[k] = packed, step
            remote(gpt.at[k], gpr.at[z], out_s, gp_r, target(k)).start()
            remote(gpk.at[k], gpkr.at[z], out_s, gp_r, target(k)).start()

        @pl.when(jnp.logical_not(away))
        def _():
            gpr[k], gpkr[k] = packed, step

    settle(d_r, packed_bytes)

    @pl.when(c == 1)
    def _():
        gq_across(unpack(gqr, gqkr, 0))

    for j in (0, 1):
        settle(gq_r.at[j], packed_bytes)
    total = gqp[x, span(y, n), :] + unpack(gqr, gqkr, 1) + unpack(gqr, gqkr, 2)
    gq_ref[...] = total + unpack(gqr, gqkr, 0) * (1 - c).astype(F32)

    def per_count(body):
        @pl.when(own)
        def _():
            body(Z - 1)

        @pl.when(crossed)
        def _():
            body(Z)

    per_count(lambda count: settle(gp_r, count * packed_bytes))
    gp_ref[...] = sum(unpack(gpr, gpkr, k) for k in range(Z))

    per_count(lambda count: settle(out_s, sent_bytes(n, w, Z, count == Z)))


def local(queries, passages, positives):
    n, w = queries.shape
    batch_count = lax.axis_size("batch")
    Z = batch_count // 4
    scale = 1.0 / math.sqrt(w * lax.axis_size("rep"))
    rows, cols = 2 * n, Z * n
    vmem = pl.BlockSpec(memory_space=pltpu.VMEM)
    dma = pltpu.SemaphoreType.DMA
    regular = pltpu.SemaphoreType.REGULAR
    hbm = pl.BlockSpec(memory_space=pltpu.HBM)
    operands = (queries, passages, positives.reshape(batch_count, n))
    grad_queries, grad_passages = pl.pallas_call(
        functools.partial(kernel, Z, scale),
        out_shape=(
            jax.ShapeDtypeStruct((n, w), F32),
            jax.ShapeDtypeStruct((n, w), F32),
        ),
        in_specs=[hbm] * 3,
        out_specs=(vmem, vmem),
        scratch_shapes=[
            pltpu.VMEM((2, rows, w), BF16),
            pltpu.VMEM((rows, w), BF16),
            pltpu.VMEM((2, cols, w), BF16),
            pltpu.VMEM((rows, cols), F32),
            pltpu.VMEM((Z, rows, n), F32),
            pltpu.VMEM((Z, rows, n), BF16),
            pltpu.VMEM((Z, rows, n), BF16),
            pltpu.VMEM((1, 2 * rows), F32),
            pltpu.VMEM((3, 1, 2 * rows), F32),
            pltpu.VMEM((1, 2 * cols), F32),
            pltpu.VMEM((2 * Z - 1, 1, 2 * cols), F32),
            pltpu.VMEM((n, w), BF16),
            pltpu.VMEM((batch_count, n), jnp.int32),
            pltpu.VMEM((1, sent_bytes(n, w, Z) // 4), F32),
            pltpu.VMEM((2, rows, w), F32),
            pltpu.VMEM((3, n, w), I16),
            pltpu.VMEM((3, n, w), I16),
            pltpu.VMEM((3, 1, w), F32),
            pltpu.VMEM((3, 1, w), F32),
            pltpu.VMEM((Z, n, w), I16),
            pltpu.VMEM((Z, n, w), I16),
            pltpu.VMEM((Z, 1, w), F32),
            pltpu.VMEM((Z, 1, w), F32),
            regular((2,)),
            regular((Z,)),
            regular,
            dma,
            dma,
            dma((2,)),
            dma((Z,)),
            dma((Z // 2,)),
            dma,
            dma,
            dma((2,)),
            dma((2,)),
            dma,
            dma,
        ],
        compiler_params=pltpu.CompilerParams(collective_id=0, has_side_effects=True, vmem_limit_bytes=6 * 2**20 + 40 * rows * cols),
    )(*(pltpu.with_memory_space_constraint(a, pltpu.HBM) for a in operands))
    return grad_queries * scale, grad_passages * scale


def solution(mesh):
    in_specs = (P("batch", "rep"), P("batch", "rep"), P())
    out_specs = (P("batch", "rep"), P("batch", "rep"))
    return jax.shard_map(local, mesh=mesh, in_specs=in_specs, out_specs=out_specs, check_vma=False)
```
